128 devices in a mesh: lat: 32 (over y, z, core), fld: 4 (over x).
Axes of the slice: x: 4, y: 4, z: 4, core: 2. Of those that a mesh axis runs over, the one named last changes fastest.
Arguments:
- grid_fields: bfloat16 [96, 1280, 2560], P('fld', 'lat'), may hold values from -6 to 6
- assign: int32 [320], replicated, may hold values from 0 to 319, each once
- limits: int32 [3], replicated, may hold values from 60 to 319, as said below
- legendre: bfloat16 [320, 641, 640], P('lat', None, 'fld'), may hold values from -0.25 to 0.25
- synth_one: bfloat16 [320, 320, 320], P('lat'), may hold values from -0.3125 to 0.3125
- synth_two: bfloat16 [320, 160, 160], P('lat'), may hold values from -0.5 to 0.5
- synth_three: bfloat16 [320, 80, 80], P('lat'), may hold values from -0.625 to 0.625
Outputs:
- spectrum: bfloat16 [96, 2, 320, 641], P('fld', None, 'lat')
- grid_one: float32 [96, 640, 1280], P('fld', 'lat')
- grid_two: float32 [96, 320, 640], P('fld', 'lat')
- grid_three: float32 [96, 160, 320], P('fld', 'lat')
The draws below stay inside these ranges and needn't reach their ends.
Inputs may be any that keep to these rules, and one draw needn't show every extreme that they name: assign is a permutation; slot q stands for the wavenumbers assign[q] and 639 - assign[q]. limits[0] is 319, limits[2] is 60, and limits[1] lies between 120 and 159.
All inputs are finite; a program needn't handle non-finite values.
Results may differ from the reference program's by a relative error of at most 0.0077.
Values may be sent and summed in bfloat16 or wider, within the bound.
No kernel may reach another device: no remote copies, remote signals or barrier semaphores. Data moves between devices by JAX's collectives and lax.ppermute only.
A program may use at most 128 MiB of HBM per device.

```python
import math
import jax
import jax.numpy as jnp

MW = 640
NLAT = 1280
NLON = 2560
FIELDS = 96
PAIRS = 320
PACK = 641
NH = 640
MW1 = 320
MW2 = 160
MW3 = 80


def draw_limits(key, part):
    counts = jnp.array([MW // 2, MW // 4, MW // 8], dtype=jnp.int32)
    middle = jax.random.randint(key, (), 0, MW // 4 // 4, dtype=jnp.int32)
    offsets = jnp.stack([jnp.zeros((), jnp.int32), middle, jnp.full((), MW // 8 // 4, jnp.int32)])
    return counts - 1 - offsets + jnp.array([0, 0, 1], dtype=jnp.int32)


def level_of(own_key, extent, pieces, least, top_value):
    factor_of = 1.0
    for axis_at, parts in pieces:
        steps = jax.random.uniform(jax.random.fold_in(jax.random.fold_in(own_key, 6), axis_at), (parts,), jnp.float32, least / len(pieces), top_value / len(pieces))
        factor_of = factor_of * jnp.repeat(jnp.exp(steps), extent[axis_at] // parts).reshape((-1,) + (1,) * (len(extent) - 1 - axis_at))
    return factor_of


def centred(rng, shape, spread, reach, pieces=(), kind=jnp.bfloat16):
    values = spread * jax.random.normal(rng, shape, jnp.float32)
    if pieces:
        values = values * level_of(rng, shape, pieces, -0.22, 0.18)
    return jnp.clip(values, -reach, reach).astype(kind)


def setup_inputs(seed: int = 0) -> dict:
    splits = jax.random.split(jax.random.key(seed), 8)
    grid_fields = centred(splits[0], (FIELDS, NLAT, NLON), 1.0, 6.0, ((0, 4), (1, 32)))
    assign = jax.random.permutation(splits[1], PAIRS).astype(jnp.int32)
    limits = draw_limits(jax.random.fold_in(splits[7], 71), 0)
    legendre = centred(splits[3], (PAIRS, PACK, NH), NH ** -0.5, 0.25, ((0, 32), (2, 4)))
    synth_one = centred(splits[4], (PAIRS, MW1, MW1), MW1 ** -0.5, 0.3125, ((0, 32),))
    synth_two = centred(splits[5], (PAIRS, MW2, MW2), MW2 ** -0.5, 0.5, ((0, 32),))
    synth_three = centred(splits[6], (PAIRS, MW3, MW3), MW3 ** -0.5, 0.625, ((0, 32),))
    return dict(grid_fields=grid_fields, assign=assign, limits=limits, legendre=legendre, synth_one=synth_one, synth_two=synth_two, synth_three=synth_three)


def phases(lon_length, wavenums):
    places = jnp.arange(lon_length, dtype=jnp.int32)
    turn_count = places[:, None] * wavenums[None, :].astype(jnp.int32) % lon_length
    angle = turn_count.astype(jnp.float32) * (2.0 * math.pi / lon_length)
    return (jnp.cos(angle), jnp.sin(angle))

def choose_pair(values, limit_of):
    ranks = jnp.arange(values.shape[-1], dtype=jnp.int32)
    keep_mask = ranks[None, :] < limit_of[:, None]
    return jnp.where(keep_mask[None, None], values[:, :, :, 0], values[:, :, :, 1])

def select_rows(sym_prod, anti_prod, own_pairs, wave_total):
    first_rows = choose_pair(sym_prod, (wave_total + 1 - own_pairs) // 2)
    later_rows = choose_pair(anti_prod, (wave_total - own_pairs) // 2)
    return jnp.concatenate([first_rows, later_rows], axis=3)

def level_field(spectrum, own_pairs, limit, synth_table):
    half_rows = synth_table.shape[1] // 2
    sym_rows = spectrum.shape[3] // 2 + 1
    step_rows = 2 * jnp.arange(half_rows, dtype=jnp.int32)
    keep_sym = own_pairs[:, None] + step_rows[None, :] <= limit
    keep_anti = own_pairs[:, None] + 1 + step_rows[None, :] <= limit
    zero_value = jnp.zeros((), jnp.bfloat16)
    kept_sym = jnp.where(keep_sym[None, None], spectrum[..., :half_rows], zero_value)
    kept_anti = jnp.where(keep_anti[None, None], spectrum[..., sym_rows:sym_rows + half_rows], zero_value)
    even_part = jnp.einsum('fcqk,qkj->fcjq', kept_sym.astype(jnp.float32), synth_table[:, :half_rows].astype(jnp.float32))
    odd_part = jnp.einsum('fcqk,qkj->fcjq', kept_anti.astype(jnp.float32), synth_table[:, half_rows:].astype(jnp.float32))
    return jnp.concatenate([even_part + odd_part, jnp.flip(even_part - odd_part, axis=2)], axis=2).astype(jnp.bfloat16)

def inverse_table(assign, lon_length):
    cosine, sine_part = phases(lon_length, assign)
    weight = jnp.where(assign == 0, 1.0, 2.0).astype(jnp.float32) / math.sqrt(lon_length)
    return jnp.stack([cosine.T * weight[:, None], -sine_part.T * weight[:, None]], axis=0).astype(jnp.bfloat16)

def reference(grid_fields, assign, limits, legendre, synth_one, synth_two, synth_three):
    pair_total = assign.shape[0]
    wave_total = 2 * pair_total
    sym_rows = pair_total + 1
    field_count, lat_total, lon_total = grid_fields.shape
    half_lat = lat_total // 2
    wavenums = jnp.stack([assign, wave_total - 1 - assign], axis=1).reshape(-1)
    cosine, sine_part = phases(lon_total, wavenums)
    dft_scale = 1.0 / math.sqrt(lon_total)
    dft_table = jnp.stack([cosine * dft_scale, -sine_part * dft_scale], axis=1).reshape(lon_total, -1).astype(jnp.bfloat16)
    fourier = jnp.dot(grid_fields.reshape(-1, lon_total), dft_table, preferred_element_type=jnp.float32).astype(jnp.bfloat16)
    split_four = fourier.reshape(field_count, lat_total, 2, pair_total, 2).astype(jnp.float32)
    north_rows = split_four[:, :half_lat]
    south_rows = jnp.flip(split_four[:, half_lat:], axis=1)
    symmetric = (north_rows + south_rows).astype(jnp.bfloat16)
    antisym = (north_rows - south_rows).astype(jnp.bfloat16)
    sym_prod = jnp.einsum('kjcsw,srj->kcswr', symmetric.astype(jnp.float32), legendre[:, :sym_rows].astype(jnp.float32))
    anti_prod = jnp.einsum('kjcsw,srj->kcswr', antisym.astype(jnp.float32), legendre[:, sym_rows:].astype(jnp.float32))
    spectrum = select_rows(sym_prod, anti_prod, assign, wave_total).astype(jnp.bfloat16)
    grids_out = []
    for level_index, synth_table in enumerate((synth_one, synth_two, synth_three)):
        level_rows = level_field(spectrum, assign, limits[level_index], synth_table)
        inverse = inverse_table(assign, 4 * synth_table.shape[1])
        grids_out.append(jnp.einsum('fcjq,cqi->fji', level_rows.astype(jnp.float32), inverse.astype(jnp.float32)))
    return (spectrum, grids_out[0], grids_out[1], grids_out[2])
```

```python
import math

import numpy as np
import jax
import jax.numpy as jnp
from jax import lax
from jax.experimental import pallas as pl
from jax.experimental.pallas import tpu as pltpu
from jax.sharding import PartitionSpec as P

F32 = jnp.float32
BF16 = jnp.bfloat16

COS_TERMS = (
    1.0,
    -4.93480110168457,
    4.058694839477539,
    -1.3351584672927856,
    0.23502981662750244,
    -0.025358986109495163,
    0.0015939108561724424,
)
SIN_TERMS = (
    3.141592502593994,
    -5.167698860168457,
    2.5499982833862305,
    -0.5985506176948547,
    0.0807478278875351,
    -0.006089475005865097,
)

NT = (((1,), (1,)), ((), ()))
NN = (((1,), (0,)), ((), ()))
VMEM_LIMIT = 60 * 1024 * 1024


def whole(shape):
    return pl.BlockSpec(shape, lambda *_: (0,) * len(shape))


def turn(count, period):
    left = count - period * jnp.floor(count * (1.0 / period) + 0.5)
    place = left * (2.0 / period)
    square = place * place
    cosine = jnp.full_like(square, COS_TERMS[-1])
    for term in COS_TERMS[-2::-1]:
        cosine = cosine * square + term
    sine = jnp.full_like(square, SIN_TERMS[-1])
    for term in SIN_TERMS[-2::-1]:
        sine = sine * square + term
    return cosine, sine * place


def fill_table(meta_ref, column, table_ref, period, width):
    rows_total = table_ref.shape[0]
    step = 64

    def body(k, carry):
        rows = pl.ds(pl.multiple_of(k * step, step), step)
        meta = meta_ref[rows, :]
        wave = meta[:, column : column + 1]
        shift = meta[:, column + 1 : column + 2]
        scale = meta[:, column + 2 : column + 3]
        lane = lax.broadcasted_iota(jnp.int32, (step, 128), 1).astype(F32)
        cos_low, sin_low = turn(lane * wave, period)
        cos_high, sin_high = turn(lane * (wave * 128.0) + shift, period)
        cos_high = cos_high * scale
        sin_high = sin_high * scale
        for a in range(-(-width // 128)):
            size = min(128, width - 128 * a)
            value = cos_high[:, a : a + 1] * cos_low - sin_high[:, a : a + 1] * sin_low
            table_ref[rows, 128 * a : 128 * a + size] = value[:, :size].astype(BF16)
        return carry

    lax.fori_loop(0, rows_total // step, body, 0)


def dft_kernel(meta_ref, grid_ref, out_ref, even_ref, odd_ref, add_ref, sub_ref):
    half = grid_ref.shape[1] // 2
    rows = grid_ref.shape[0]
    fill_table(meta_ref, 0, even_ref, 2 * half, half)
    fill_table(meta_ref, 3, odd_ref, 2 * half, half)

    def fold(k, carry):
        part = pl.ds(pl.multiple_of(k * 64, 64), 64)
        first = grid_ref[part, :half].astype(F32)
        second = grid_ref[part, half:].astype(F32)
        add_ref[part, :] = (first + second).astype(BF16)
        sub_ref[part, :] = (first - second).astype(BF16)
        return carry

    lax.fori_loop(0, rows // 64, fold, 0)

    def block(k, carry):
        part = pl.ds(pl.multiple_of(k * 192, 192), 192)
        even = lax.dot_general(even_ref[part, :], add_ref[...], NT, preferred_element_type=F32)
        odd = lax.dot_general(odd_ref[part, :], sub_ref[...], NT, preferred_element_type=F32)
        for d in range(8):
            one = even[24 * d : 24 * d + 24]
            two = odd[24 * d : 24 * d + 24]
            value = jnp.concatenate([one[:16], one[16:] + two[:8], two[8:]], axis=0)
            out_ref[k * 8 + d, :, :rows] = value.astype(BF16)
        return carry

    lax.fori_loop(0, out_ref.shape[0] // 8, block, 0)


def lanes_kernel(wire_ref, out_ref, north_ref, south_ref):
    fields = north_ref.shape[1] // 40
    lane = lax.broadcasted_iota(jnp.int32, (8, 128), 1)

    def field(f, carry):
        base = pl.multiple_of(jnp.minimum(f * 40 // 128, 6) * 128, 128)
        offset = f * 40 - base
        rows = pl.ds(pl.multiple_of(f * 40, 8), 40)
        for half, target in ((0, north_ref), (16, south_ref)):
            for x in range(4):
                low = [jnp.zeros((8, 128), F32) for _ in range(5)]
                high = None
                for k in range(4):
                    window = wire_ref[half + 4 * x + k, :, pl.ds(base, 256)].astype(F32)
                    shift = lax.rem(40 * k - offset + 256, 128)
                    second = lane + (offset - 40 * k) >= 128
                    inside = (lane >= 40 * k) & (lane < 40 * k + 40)
                    first_rolled = pltpu.roll(window[:, :128], shift, 1)
                    next_rolled = pltpu.roll(window[:, 128:], shift, 1)
                    for t in range(5):
                        one = first_rolled[8 * t : 8 * t + 8]
                        two = next_rolled[8 * t : 8 * t + 8]
                        piece = jnp.where(second, two, one)
                        low[t] = jnp.where(inside, piece, low[t])
                    if k == 3:
                        second = lane + (offset + 8) >= 128
                        high = [
                            jnp.where(
                                lane < 32,
                                jnp.where(
                                    second,
                                    next_rolled[8 * t : 8 * t + 8],
                                    first_rolled[8 * t : 8 * t + 8],
                                ),
                                0.0,
                            )
                            for t in range(5)
                        ]
                target[2 * x, rows, :] = jnp.concatenate(low, axis=0)
                target[2 * x + 1, rows, :] = jnp.concatenate(high, axis=0)
        return carry

    lax.fori_loop(0, fields, field, 0)

    across = lax.broadcasted_iota(jnp.int32, (256, 256), 0)
    along = lax.broadcasted_iota(jnp.int32, (256, 256), 1)
    mirror = jnp.where(across + along == 159, 1.0, 0.0).astype(BF16)

    def fold(k, carry):
        rows = pl.ds(pl.multiple_of(k * 96, 96), 96)
        south = [
            lax.dot_general(
                jnp.concatenate(
                    [south_ref[6 - 2 * x, rows, :], south_ref[7 - 2 * x, rows, :]], axis=1
                ).astype(BF16),
                mirror,
                NN,
                preferred_element_type=F32,
            )
            for x in range(4)
        ]
        for t in range(8):
            second = south[t // 2][:, t % 2 * 128 : t % 2 * 128 + 128]
            first = north_ref[t, rows, :]
            north_ref[t, rows, :] = first + second
            south_ref[t, rows, :] = first - second
        return carry

    lax.fori_loop(0, north_ref.shape[1] // 96, fold, 0)

    def slot(q, carry):
        for x in range(4):
            for t in range(2):
                parts = [
                    source[2 * x + t, pl.ds(g * 10 + q, fields, stride=40), :]
                    for source in (north_ref, south_ref)
                    for g in range(4)
                ]
                part = jnp.concatenate(parts, axis=0).astype(BF16)
                if t:
                    out_ref[q, x, :, 128:] = part[:, :32]
                else:
                    out_ref[q, x, :, :128] = part
        return carry

    lax.fori_loop(0, out_ref.shape[0], slot, 0)


def turn_tables_kernel(one_ref, two_ref, three_ref, out_one, out_two, out_three):
    for source, target, groups in ((one_ref, out_one, 4), (two_ref, out_two, 2), (three_ref, out_three, 1)):
        size = source.shape[1]
        row = lax.broadcasted_iota(jnp.int32, (size, size), 0)
        column = lax.broadcasted_iota(jnp.int32, (size, size), 1)
        b = row // (16 * groups)
        a = (row // 16) % groups
        place = (row % 16) * (5 * groups) + 5 * a + b
        pick = jnp.where(place == column, 1.0, 0.0).astype(BF16)
        target[0] = lax.dot_general(pick, source[0], NT, preferred_element_type=F32).astype(BF16)


def slot_kernel(
    info_ref,
    waves_ref,
    own_ref,
    left_ref,
    right_ref,
    far_low_ref,
    far_high_ref,
    one_ref,
    two_ref,
    three_ref,
    spectrum_ref,
    wire_ref,
    row_ref,
    pack_ref,
):
    q = pl.program_id(0)
    x = info_ref[0]
    p = info_ref[1 + q]

    @pl.when(q == 0)
    def _():
        row_ref[...] = jnp.zeros_like(row_ref)
        pack_ref[...] = jnp.zeros_like(pack_ref)

    far = jnp.where(q < 5, far_low_ref[0], far_high_ref[0])
    total = lax.dot_general(waves_ref[0, x], own_ref[0], NN, preferred_element_type=F32)
    for step, block in ((3, left_ref[0]), (1, right_ref[0]), (2, far)):
        total += lax.dot_general(
            waves_ref[0, (x + step) % 4], block, NN, preferred_element_type=F32
        )
    rank = lax.broadcasted_iota(jnp.int32, (48, 641), 1)
    even_pair = p % 2 == 0
    sym = rank < 321
    place = jnp.where(sym, rank, rank - 321)
    bound = jnp.where(sym, (641 - p) // 2, (640 - p) // 2)
    first = (place < bound) == even_pair
    chosen = jnp.where(
        sym,
        jnp.where(first, total[0:48], total[48:96]),
        jnp.where(first, total[96:144], total[144:192]),
    ).astype(BF16)
    spectrum_ref[0] = chosen
    row_ref[:, :641] = chosen.astype(F32)
    rows = row_ref[...]
    group = 0
    for level, table_ref, count in ((0, one_ref, 4), (1, two_ref, 2), (2, three_ref, 1)):
        size = table_ref.shape[1]
        half = size // 2
        limit = info_ref[11 + level]
        lane = lax.broadcasted_iota(jnp.int32, (48, size), 1)
        is_sym = lane < half
        later = pltpu.roll(rows, 768 - 321 + half, 1)[:, :size]
        order = p + jnp.where(is_sym, 2 * lane, 2 * (lane - half) + 1)
        kept = jnp.where(order <= limit, jnp.where(is_sym, rows[:, :size], later), 0.0)
        both = jnp.concatenate(
            [kept, jnp.where(is_sym, kept, -kept), jnp.zeros((32, size), F32)], axis=0
        ).astype(BF16)
        value = lax.dot_general(table_ref[0], both, NT, preferred_element_type=F32)
        many = 16 * count
        lane = lax.broadcasted_iota(jnp.int32, (many, 128), 1)
        for sign in range(2):
            for c in range(2):
                packed = jnp.zeros((many, 128), F32)
                for b in range(5):
                    part = value[many * b : many * b + many]
                    move = 24 * (b - 2 * sign - c) % 128
                    if move:
                        part = pltpu.roll(part, move, 1)
                    packed = jnp.where((lane >= 24 * b) & (lane < 24 * b + 24), part, packed)
                for a in range(count):
                    start = sign * 16 * 144 + 20 * (group + a) + 10 * c + q
                    pack_ref[pl.ds(start, 16, stride=144), :] = packed[16 * a : 16 * a + 16]
        group += count

    @pl.when(q == pl.num_programs(0) - 1)
    def _():
        for d in range(16):
            wire_ref[d] = pack_ref[144 * d : 144 * d + 144, :].astype(BF16)
            wire_ref[31 - d] = pack_ref[144 * (16 + d) : 144 * (17 + d), :].astype(BF16)


def inverse_table_kernel(meta_ref, one_ref, one_late_ref, two_ref, two_late_ref, three_ref):
    fill_table(meta_ref, 0, one_ref, 1280, 1280)
    fill_table(meta_ref, 3, one_late_ref, 1280, 1280)
    fill_table(meta_ref, 6, two_ref, 640, 640)
    fill_table(meta_ref, 9, two_late_ref, 640, 640)
    fill_table(meta_ref, 12, three_ref, 320, 320)


def inverse_kernel(
    info_ref,
    wire_ref,
    one_ref,
    one_late_ref,
    two_ref,
    two_late_ref,
    three_ref,
    out_one,
    out_two,
    out_three,
):
    late_half = info_ref[0]
    across = lax.broadcasted_iota(jnp.int32, (128, 128), 0)
    along = lax.broadcasted_iota(jnp.int32, (128, 128), 1)
    same = jnp.where(across == along, 1.0, 0.0).astype(BF16)

    def lines(group):
        start = 20 * group // 8 * 8
        part = wire_ref[:, start : start + 24, :].astype(F32)
        part = part.reshape(part.shape[0] * 24, 128).astype(BF16)
        return lax.dot_general(same, part, NT, preferred_element_type=F32).astype(BF16)

    def place(target, a, value):
        last = target.shape[0] - 1
        for b in range(5):
            row = 5 * a + b
            row = jnp.where(late_half == 1, last - row, row)
            target[row] = value[24 * b : 24 * b + 24]

    for target, tables, group, count in (
        (out_one, (one_ref, one_late_ref), 0, 4),
        (out_two, (two_ref, two_late_ref), 4, 2),
        (out_three, (three_ref,), 6, 1),
    ):
        for late, table in enumerate(tables):
            members = [a for a in range(count) if (group + a) % 2 == late]
            left = [lines(group + a) for a in members]
            left = jnp.concatenate(left, axis=0) if len(left) > 1 else left[0]
            value = lax.dot_general(left, table[...], NN, preferred_element_type=F32)
            for k, a in enumerate(members):
                place(target, a, value[128 * k : 128 * k + 128])


def call(kernel, out_shape, **kw):
    return pl.pallas_call(
        kernel,
        out_shape=out_shape,
        compiler_params=pltpu.CompilerParams(vmem_limit_bytes=VMEM_LIMIT),
        **kw,
    )


def spread(pairs, early):
    spare = jnp.zeros((pairs.shape[0], 4), F32)
    parts = [pairs, pairs, spare] if early else [spare, pairs, pairs]
    return jnp.concatenate(parts, axis=1).reshape(-1)


def steady(first, second, early):
    parts = [first] * 10 + [second] * 10
    parts = parts + [0.0] * 4 if early else [0.0] * 4 + parts
    return jnp.asarray(np.tile(np.asarray(parts, np.float32), 32))


def on_device(grid_fields, assign, limits, legendre, synth_one, synth_two, synth_three):
    fields, rows, lon = grid_fields.shape
    lat_at = lax.axis_index("lat")
    fld_at = lax.axis_index("fld")
    pairs = assign.reshape(32, 10)
    even = jnp.where(pairs % 2 == 0, pairs, 639 - pairs).astype(F32)
    odd = 639.0 - even
    scale = 1.0 / math.sqrt(lon)
    meta = jnp.stack(
        [
            spread(even, True),
            steady(0.0, lon / 4.0, True),
            steady(scale, scale, True),
            spread(odd, False),
            steady(0.0, lon / 4.0, False),
            steady(scale, scale, False),
        ],
        axis=1,
    )

    own = jnp.transpose(legendre, (0, 2, 1))
    right = [(k, (k + 1) % 4) for k in range(4)]
    left = [(k, (k + 3) % 4) for k in range(4)]
    from_left = lax.ppermute(own, "fld", right)
    from_right = lax.ppermute(own, "fld", left)
    far_low = lax.ppermute(from_left[:5], "fld", right)
    far_high = lax.ppermute(from_right[5:], "fld", left)

    wire = call(
        dft_kernel,
        jax.ShapeDtypeStruct((32, 40, 1024), BF16),
        scratch_shapes=[
            pltpu.VMEM((768, lon // 2), BF16),
            pltpu.VMEM((768, lon // 2), BF16),
            pltpu.VMEM((fields * rows, lon // 2), BF16),
            pltpu.VMEM((fields * rows, lon // 2), BF16),
        ],
        name="dft",
    )(meta, grid_fields.reshape(fields * rows, lon))
    assign_after, synth_one, synth_two, synth_three, wire = lax.optimization_barrier(
        (assign, synth_one, synth_two, synth_three, wire)
    )
    wire = lax.all_to_all(wire, "lat", split_axis=0, concat_axis=0, tiled=True)

    turned = call(
        turn_tables_kernel,
        [jax.ShapeDtypeStruct(t.shape, BF16) for t in (synth_one, synth_two, synth_three)],
        grid=(10,),
        in_specs=[
            pl.BlockSpec((1,) + t.shape[1:], lambda q: (q, 0, 0))
            for t in (synth_one, synth_two, synth_three)
        ],
        out_specs=[
            pl.BlockSpec((1,) + t.shape[1:], lambda q: (q, 0, 0))
            for t in (synth_one, synth_two, synth_three)
        ],
        name="turn_tables",
    )(synth_one, synth_two, synth_three)

    pairs = assign_after.reshape(32, 10)
    plain = pairs.astype(F32)
    weight = jnp.where(pairs == 0, 1.0, 2.0).astype(F32)
    columns = []
    for size in (1280, 640, 320):
        for early in (True, False) if size > 320 else (True,):
            columns += [
                spread(plain, early),
                steady(0.0, size / 4.0, early),
                spread(weight * (1.0 / math.sqrt(size)), early),
            ]
    inverse_meta = jnp.stack(columns, axis=1)
    tables = call(
        inverse_table_kernel,
        [jax.ShapeDtypeStruct((768, n), BF16) for n in (1280, 1280, 640, 640, 320)],
        name="inverse_tables",
    )(inverse_meta)

    waves = call(
        lanes_kernel,
        jax.ShapeDtypeStruct((10, 4, 192, 160), BF16),
        scratch_shapes=[
            pltpu.VMEM((8, fields * rows, 128), F32),
            pltpu.VMEM((8, fields * rows, 128), F32),
        ],
        name="lanes",
    )(wire)

    info = jnp.concatenate(
        [
            fld_at.reshape(1),
            lax.dynamic_slice_in_dim(assign, lat_at * 10, 10),
            limits,
        ]
    )
    block = pl.BlockSpec((1, 160, 641), lambda q, *_: (q, 0, 0))
    spectrum, level_wire = call(
        slot_kernel,
        [
            jax.ShapeDtypeStruct((10, 2 * fields, 641), BF16),
            jax.ShapeDtypeStruct((32, 144, 128), BF16),
        ],
        grid_spec=pltpu.PrefetchScalarGridSpec(
            num_scalar_prefetch=1,
            grid=(10,),
            in_specs=[
                pl.BlockSpec((1, 4, 192, 160), lambda q, *_: (q, 0, 0, 0)),
                block,
                block,
                block,
                pl.BlockSpec((1, 160, 641), lambda q, *_: (jnp.minimum(q, 4), 0, 0)),
                pl.BlockSpec((1, 160, 641), lambda q, *_: (jnp.maximum(q - 5, 0), 0, 0)),
            ]
            + [pl.BlockSpec((1,) + t.shape[1:], lambda q, *_: (q, 0, 0)) for t in turned],
            out_specs=[
                pl.BlockSpec((1, 2 * fields, 641), lambda q, *_: (q, 0, 0)),
                pl.BlockSpec((32, 144, 128), lambda q, *_: (0, 0, 0)),
            ],
            scratch_shapes=[
                pltpu.VMEM((48, 768), F32),
                pltpu.VMEM((32 * 144, 128), F32),
            ],
        ),
        name="slots",
    )(info, waves, own, from_left, from_right, far_low, far_high, *turned)

    level_wire = lax.all_to_all(level_wire, "lat", split_axis=0, concat_axis=0, tiled=True)
    late_half = (lat_at >= 16).astype(jnp.int32).reshape(1)
    vmem = pl.BlockSpec(memory_space=pltpu.VMEM)
    grids = call(
        inverse_kernel,
        [
            jax.ShapeDtypeStruct((20, fields, 1280), F32),
            jax.ShapeDtypeStruct((10, fields, 640), F32),
            jax.ShapeDtypeStruct((5, fields, 320), F32),
        ],
        in_specs=[pl.BlockSpec(memory_space=pltpu.SMEM)] + [vmem] * 6,
        out_specs=[vmem] * 3,
        name="inverse",
    )(late_half, level_wire, *tables)
    grids = [jnp.transpose(g, (1, 0, 2)) for g in grids]
    spectrum = jnp.transpose(spectrum.reshape(10, 2, fields, 641), (2, 1, 0, 3))
    return (spectrum, *grids)


def solution(mesh):
    return jax.shard_map(
        on_device,
        mesh=mesh,
        in_specs=(
            P("fld", "lat", None),
            P(),
            P(),
            P("lat", None, "fld"),
            P("lat", None, None),
            P("lat", None, None),
            P("lat", None, None),
        ),
        out_specs=(
            P("fld", None, "lat", None),
            P("fld", "lat", None),
            P("fld", "lat", None),
            P("fld", "lat", None),
        ),
        check_vma=False,
    )
```

```python
import functools
import math

import jax
import jax.numpy as jnp
from jax import lax
from jax.experimental import pallas as pl
from jax.experimental.pallas import tpu as pltpu
from jax.sharding import PartitionSpec as P

F32 = jnp.float32
BF16 = jnp.bfloat16

COS_TERMS = (
    1.0,
    -4.93480110168457,
    4.058694839477539,
    -1.3351584672927856,
    0.23502981662750244,
    -0.025358986109495163,
    0.0015939108561724424,
)
SIN_TERMS = (
    3.141592502593994,
    -5.167698860168457,
    2.5499982833862305,
    -0.5985506176948547,
    0.0807478278875351,
    -0.006089475005865097,
)

NT = (((1,), (1,)), ((), ()))
NN = (((1,), (0,)), ((), ()))


def whole(shape):
    return pl.BlockSpec(shape, lambda *_: (0,) * len(shape))


def turn(count, period):
    left = count - period * jnp.floor(count * (1.0 / period) + 0.5)
    place = left * (2.0 / period)
    square = place * place
    cosine = jnp.full_like(square, COS_TERMS[-1])
    for term in COS_TERMS[-2::-1]:
        cosine = cosine * square + term
    sine = jnp.full_like(square, SIN_TERMS[-1])
    for term in SIN_TERMS[-2::-1]:
        sine = sine * square + term
    return cosine, sine * place


def fill_table(wave, shift, scale, high_cos, high_sin, table_ref, period):
    count, width = table_ref.shape
    step = 16
    many = count // step
    low = lax.broadcasted_iota(jnp.int32, (step, width), 0).astype(F32)
    low_cos, low_sin = turn(low * wave, period)
    high = lax.broadcasted_iota(jnp.int32, (many, width), 0).astype(F32)
    first, second = turn(high * (wave * float(step)) + shift, period)
    high_cos[:many, :] = first * scale
    high_sin[:many, :] = second * scale

    def body(k, carry):
        value = high_cos[pl.ds(k, 1), :] * low_cos - high_sin[pl.ds(k, 1), :] * low_sin
        table_ref[pl.ds(pl.multiple_of(k * step, step), step), :] = value.astype(BF16)
        return carry

    lax.fori_loop(0, many, body, 0)


def identity(size):
    across = lax.broadcasted_iota(jnp.int32, (size, size), 0)
    along = lax.broadcasted_iota(jnp.int32, (size, size), 1)
    return jnp.where(across == along, 1.0, 0.0).astype(BF16)


def dft_kernel(waves_ref, grid_ref, out_ref, even_ref, odd_ref, add_ref, sub_ref, turned_ref, high_cos, high_sin):
    half = grid_ref.shape[1] // 2
    rows = grid_ref.shape[0]
    lane = lax.broadcasted_iota(jnp.int32, (1, 768), 1).astype(F32)
    lane = lane - 24.0 * jnp.floor((lane + 0.5) * (1.0 / 24.0))
    size = 1.0 / math.sqrt(2 * half)
    for at, table_ref, first in ((0, even_ref, 0.0), (1, odd_ref, 4.0)):
        valid = (lane >= first) & (lane < first + 20.0)
        fill_table(
            waves_ref[at : at + 1, :],
            jnp.where(lane >= first + 10.0, half / 2.0, 0.0),
            jnp.where(valid, size, 0.0),
            high_cos,
            high_sin,
            table_ref,
            2 * half,
        )

    def fold(k, carry):
        part = pl.ds(pl.multiple_of(k * 64, 64), 64)
        first = grid_ref[part, :half].astype(F32)
        second = grid_ref[part, half:].astype(F32)
        add_ref[part, :] = (first + second).astype(BF16)
        sub_ref[part, :] = (first - second).astype(BF16)
        return carry

    lax.fori_loop(0, rows // 64, fold, 0)
    same = identity(128)

    def block(k, carry):
        results = []
        for table_ref, folded_ref in ((even_ref, add_ref), (odd_ref, sub_ref)):
            for t in range(3):
                columns = pl.ds(pl.multiple_of(k * 384 + 128 * t, 128), 128)
                turned_ref[128 * t : 128 * t + 128, :] = lax.dot_general(
                    same, table_ref[:, columns], NT, preferred_element_type=F32
                ).astype(BF16)
            results.append(
                lax.dot_general(turned_ref[...], folded_ref[...], NT, preferred_element_type=F32)
            )
        even, odd = results
        for d in range(16):
            one = even[24 * d : 24 * d + 24]
            two = odd[24 * d : 24 * d + 24]
            value = jnp.concatenate([one[:16], one[16:] + two[:8], two[8:]], axis=0)
            out_ref[k * 16 + d, :, :rows] = value.astype(BF16)
        return carry

    lax.fori_loop(0, out_ref.shape[0] // 16, block, 0)


def pack_kernel(block_ref, low_ref, high_ref, last_ref):
    q = pl.program_id(0)
    value = block_ref[0]
    lane = lax.broadcasted_iota(jnp.int32, (160, 128), 1)
    last = jnp.where(lane == 0, value[:, 640:].astype(F32), 0.0)
    last = pltpu.roll(last, q, 1)

    @pl.when(q == 0)
    def _():
        last_ref[...] = last

    @pl.when(q > 0)
    def _():
        last_ref[...] += last

    @pl.when(q < 5)
    def _():
        low_ref[pl.ds(pl.multiple_of(q * 160, 160), 160), :] = value[:, :640]

    @pl.when(q >= 5)
    def _():
        high_ref[pl.ds(pl.multiple_of(q * 160 - 800, 160), 160), :] = value[:, :640]

    @pl.when(q == 9)
    def _():
        for t in range(5):
            low_ref[800:832, 128 * t : 128 * t + 128] = last_ref[32 * t : 32 * t + 32, :].astype(BF16)


def lanes_kernel(wire_ref, out_ref, north_ref, south_ref):
    fields = north_ref.shape[1] // 40
    lane = lax.broadcasted_iota(jnp.int32, (40, 128), 1)

    def field(f, carry):
        base = pl.multiple_of(jnp.minimum(f * 40 // 128, 6) * 128, 128)
        offset = f * 40 - base
        rows = pl.ds(pl.multiple_of(f * 40, 8), 40)
        for half, target in ((0, north_ref), (16, south_ref)):
            for x in range(4):
                low = None
                for k in range(4):
                    window = wire_ref[half + 4 * x + k, :, pl.ds(base, 256)]
                    shift = lax.rem(40 * k - offset + 256, 128)
                    first = pltpu.roll(window[:, :128], shift, 1)
                    second = pltpu.roll(window[:, 128:], shift, 1)
                    piece = jnp.where(lane + (offset - 40 * k) >= 128, second, first)
                    low = piece if low is None else jnp.where(lane >= 40 * k, piece, low)
                high = jnp.where(lane + (offset + 8) >= 128, second, first)
                high = jnp.where(lane < 32, high, jnp.zeros_like(high))
                target[2 * x, rows, :] = low.astype(F32)
                target[2 * x + 1, rows, :] = high.astype(F32)
        return carry

    lax.fori_loop(0, fields, field, 0)

    across = lax.broadcasted_iota(jnp.int32, (256, 256), 0)
    along = lax.broadcasted_iota(jnp.int32, (256, 256), 1)
    mirror = jnp.where(across + along == 159, 1.0, 0.0).astype(BF16)

    def fold(k, carry):
        rows = pl.ds(pl.multiple_of(k * 96, 96), 96)
        south = [
            lax.dot_general(
                jnp.concatenate(
                    [south_ref[6 - 2 * x, rows, :], south_ref[7 - 2 * x, rows, :]], axis=1
                ).astype(BF16),
                mirror,
                NN,
                preferred_element_type=F32,
            )
            for x in range(4)
        ]
        for t in range(8):
            second = south[t // 2][:, t % 2 * 128 : t % 2 * 128 + 128]
            first = north_ref[t, rows, :]
            north_ref[t, rows, :] = first + second
            south_ref[t, rows, :] = first - second
        return carry

    lax.fori_loop(0, north_ref.shape[1] // 96, fold, 0)

    def slot(q, carry):
        for x in range(4):
            for t in range(2):
                parts = [
                    source[2 * x + t, pl.ds(g * 10 + q, fields, stride=40), :]
                    for source in (north_ref, south_ref)
                    for g in range(4)
                ]
                part = jnp.concatenate(parts, axis=0).astype(BF16)
                if t:
                    out_ref[q, x, :, 128:] = part[:, :32]
                else:
                    out_ref[q, x, :, :128] = part
        return carry

    lax.fori_loop(0, out_ref.shape[0], slot, 0)


def turn_tables_kernel(one_ref, two_ref, three_ref, out_one, out_two, out_three, *picks):
    levels = ((one_ref, out_one, 4), (two_ref, out_two, 2), (three_ref, out_three, 1))

    @pl.when(pl.program_id(0) == 0)
    def _():
        for pick_ref, (source, _, groups) in zip(picks, levels):
            size = source.shape[1]
            row = lax.broadcasted_iota(jnp.int32, (size, size), 0)
            column = lax.broadcasted_iota(jnp.int32, (size, size), 1)
            b = row // (16 * groups)
            a = (row // 16) % groups
            place = (row % 16) * (5 * groups) + 5 * a + b
            pick_ref[...] = jnp.where(place == column, 1.0, 0.0).astype(BF16)

    for pick_ref, (source, target, _) in zip(picks, levels):
        target[0] = lax.dot_general(
            pick_ref[...], source[0], NT, preferred_element_type=F32
        ).astype(BF16)


def slot_kernel(
    first_slot,
    info_ref,
    waves_ref,
    own_ref,
    left_ref,
    right_ref,
    far_ref,
    own_last,
    left_last,
    right_last,
    far_last,
    one_ref,
    two_ref,
    three_ref,
    spectrum_ref,
    wire_ref,
    pack_ref,
):
    q = pl.program_id(0)
    slot = q + first_slot
    x = info_ref[0]
    p = info_ref[1 + slot]

    @pl.when(q == 0)
    def _():
        for row in (70, 71):
            pack_ref[pl.ds(row, 32, stride=72), :] = jnp.zeros((32, 128), F32)

    total = None
    for step, block_ref, last_ref in (
        (0, own_ref, own_last),
        (3, left_ref, left_last),
        (1, right_ref, right_last),
        (2, far_ref, far_last),
    ):
        last = jnp.concatenate([last_ref[:, 128 * t : 128 * t + 128] for t in range(5)], axis=0)
        block = jnp.concatenate([block_ref[...], last], axis=1)
        term = lax.dot_general(
            waves_ref[0, (x + step) % 4], block, NN, preferred_element_type=F32
        )
        total = term if total is None else total + term
    total = jnp.concatenate(
        [total[:, :640], pltpu.roll(total[:, 640:], lax.rem(128 - slot, 128), 1)], axis=1
    )
    rank = lax.broadcasted_iota(jnp.int32, (48, 768), 1)
    even_pair = p % 2 == 0
    sym = rank < 321
    place = jnp.where(sym, rank, rank - 321)
    bound = jnp.where(sym, (641 - p) // 2, (640 - p) // 2)
    first = (place < bound) == even_pair
    chosen = jnp.where(
        sym,
        jnp.where(first, total[0:48], total[48:96]),
        jnp.where(first, total[96:144], total[144:192]),
    ).astype(BF16)
    spectrum_ref[0] = chosen[:, :641]
    rows = chosen.astype(F32)
    group = 0
    for level, table_ref, count in ((0, one_ref, 4), (1, two_ref, 2), (2, three_ref, 1)):
        size = table_ref.shape[1]
        half = size // 2
        limit = info_ref[11 + level]
        lane = lax.broadcasted_iota(jnp.int32, (48, size), 1)
        is_sym = lane < half
        later = pltpu.roll(rows, 768 - 321 + half, 1)[:, :size]
        order = p + jnp.where(is_sym, 2 * lane, 2 * (lane - half) + 1)
        kept = jnp.where(order <= limit, jnp.where(is_sym, rows[:, :size], later), 0.0)
        both = jnp.concatenate(
            [kept, jnp.where(is_sym, kept, -kept), jnp.zeros((32, size), F32)], axis=0
        ).astype(BF16)
        value = lax.dot_general(table_ref[0], both, NT, preferred_element_type=F32)
        many = 16 * count
        lane = lax.broadcasted_iota(jnp.int32, (many, 128), 1)
        for sign in range(2):
            for c in range(2):
                packed = jnp.zeros((many, 128), F32)
                for b in range(5):
                    part = value[many * b : many * b + many]
                    move = 24 * (b - 2 * sign - c) % 128
                    if move:
                        part = pltpu.roll(part, move, 1)
                    packed = jnp.where((lane >= 24 * b) & (lane < 24 * b + 24), part, packed)
                for a in range(count):
                    start = sign * 16 * 72 + 10 * (group + a) + 5 * c + q
                    pack_ref[pl.ds(start, 16, stride=72), :] = packed[16 * a : 16 * a + 16]
        group += count

    @pl.when(q == pl.num_programs(0) - 1)
    def _():
        for d in range(16):
            wire_ref[d] = pack_ref[72 * d : 72 * d + 72, :].astype(BF16)
            wire_ref[31 - d] = pack_ref[72 * (16 + d) : 72 * (17 + d), :].astype(BF16)


def inverse_table_kernel(waves_ref, one_ref, two_ref, three_ref, high_cos, high_sin):
    wave = waves_ref[0:1, :]
    lane = lax.broadcasted_iota(jnp.int32, (1, 1024), 1) & 15
    weight = jnp.where(lane < 10, jnp.where(wave == 0.0, 1.0, 2.0), 0.0)
    for table_ref in (one_ref, two_ref, three_ref):
        period = table_ref.shape[0]
        shift = jnp.where(lane >= 5, period / 4.0, 0.0)
        scale = weight * (1.0 / math.sqrt(period))
        fill_table(wave, shift, scale, high_cos, high_sin, table_ref, period)


def inverse_kernel(
    info_ref, low_ref, high_ref, one_ref, two_ref, three_ref, out_one, out_two, out_three
):
    late_half = info_ref[0]
    same = identity(128)

    def lines(group):
        start = 10 * group // 8 * 8
        parts = []
        for wire_ref in (low_ref, high_ref):
            part = wire_ref[:, start : start + 16, :].astype(F32)
            if 10 * group > start:
                part = pltpu.roll(part, 16 - (10 * group - start), 1)
            parts.append(part)
        part = jnp.concatenate(parts, axis=1)
        part = part.reshape(part.shape[0] * 32, 128).astype(BF16)
        return lax.dot_general(same, part, NT, preferred_element_type=F32).astype(BF16)

    for target, table, group, count in (
        (out_one, one_ref, 0, 4),
        (out_two, two_ref, 4, 2),
        (out_three, three_ref, 6, 1),
    ):
        left = [lines(group + a) for a in range(count)]
        left = jnp.concatenate(left, axis=0) if count > 1 else left[0]
        value = lax.dot_general(left, table[...], NT, preferred_element_type=F32)
        last = target.shape[0] - 1
        for a in range(count):
            for b in range(5):
                row = 5 * a + b
                row = jnp.where(late_half == 1, last - row, row)
                target[row] = value[128 * a + 24 * b : 128 * a + 24 * b + 24]


def call(kernel, out_shape, limit, **kw):
    return pl.pallas_call(
        kernel,
        out_shape=out_shape,
        compiler_params=pltpu.CompilerParams(vmem_limit_bytes=limit * 1024 * 1024),
        **kw,
    )


def on_device(grid_fields, assign, limits, legendre, synth_one, synth_two, synth_three):
    fields, rows, lon = grid_fields.shape
    lat_at = lax.axis_index("lat")
    fld_at = lax.axis_index("fld")
    vmem = pl.BlockSpec(memory_space=pltpu.VMEM)

    own = jnp.transpose(legendre, (0, 2, 1))
    low, high = call(
        pack_kernel,
        [jax.ShapeDtypeStruct((832, 640), BF16), jax.ShapeDtypeStruct((800, 640), BF16)],
        8,
        grid=(10,),
        in_specs=[pl.BlockSpec((1, 160, 641), lambda q: (q, 0, 0))],
        out_specs=[whole((832, 640)), whole((800, 640))],
        scratch_shapes=[pltpu.VMEM((160, 128), F32)],
        name="pack",
    )(own)
    right = [(k, (k + 1) % 4) for k in range(4)]
    left = [(k, (k + 3) % 4) for k in range(4)]
    low_left = lax.ppermute(low, "fld", right)
    high_right = lax.ppermute(high, "fld", left)
    low_right = lax.ppermute(low, "fld", left)
    high_left = lax.ppermute(high, "fld", right)
    low_far = lax.ppermute(low_left, "fld", right)
    high_far = lax.ppermute(high_right, "fld", left)

    pairs = assign.reshape(32, 10)
    even = jnp.where(pairs % 2 == 0, pairs, 639 - pairs).astype(F32)
    odd = 639.0 - even
    spare = jnp.zeros((32, 4), F32)
    forward_waves = jnp.stack(
        [
            jnp.concatenate([even, even, spare], axis=1),
            jnp.concatenate([spare, odd, odd], axis=1),
        ]
    ).reshape(2, 768)
    wire = call(
        dft_kernel,
        jax.ShapeDtypeStruct((32, 40, 1024), BF16),
        32,
        in_specs=[vmem, vmem],
        out_specs=vmem,
        scratch_shapes=[
            pltpu.VMEM((lon // 2, 768), BF16),
            pltpu.VMEM((lon // 2, 768), BF16),
            pltpu.VMEM((fields * rows, lon // 2), BF16),
            pltpu.VMEM((fields * rows, lon // 2), BF16),
            pltpu.VMEM((384, lon // 2), BF16),
            pltpu.VMEM((80, 768), F32),
            pltpu.VMEM((80, 768), F32),
        ],
        name="dft",
    )(forward_waves, grid_fields.reshape(fields * rows, lon))
    assign_after, synth_one, synth_two, synth_three, wire = lax.optimization_barrier(
        (assign, synth_one, synth_two, synth_three, wire)
    )
    wire = lax.all_to_all(wire, "lat", split_axis=0, concat_axis=0, tiled=True)

    synths = (synth_one, synth_two, synth_three)
    slot_block = [pl.BlockSpec((1,) + t.shape[1:], lambda q: (q, 0, 0)) for t in synths]
    turned = call(
        turn_tables_kernel,
        [jax.ShapeDtypeStruct(t.shape, BF16) for t in synths],
        8,
        grid=(10,),
        in_specs=slot_block,
        out_specs=slot_block,
        scratch_shapes=[pltpu.VMEM(t.shape[1:], BF16) for t in synths],
        name="turn_tables",
    )(*synths)

    plain = assign_after.reshape(32, 10).astype(F32)
    spare = jnp.zeros((32, 6), F32)
    one, two = plain[:, :5], plain[:, 5:]
    inverse_waves = jnp.concatenate([one, one, spare, two, two, spare], axis=1).reshape(1, 1024)
    tables = call(
        inverse_table_kernel,
        [jax.ShapeDtypeStruct((n, 1024), BF16) for n in (1280, 640, 320)],
        12,
        in_specs=[vmem],
        out_specs=[vmem] * 3,
        scratch_shapes=[pltpu.VMEM((80, 1024), F32), pltpu.VMEM((80, 1024), F32)],
        name="inverse_tables",
    )(inverse_waves)

    waves = call(
        lanes_kernel,
        jax.ShapeDtypeStruct((10, 4, 192, 160), BF16),
        22,
        in_specs=[vmem],
        out_specs=vmem,
        scratch_shapes=[
            pltpu.VMEM((8, fields * rows, 128), F32),
            pltpu.VMEM((8, fields * rows, 128), F32),
        ],
        name="lanes",
    )(wire)

    info = jnp.concatenate(
        [fld_at.reshape(1), lax.dynamic_slice_in_dim(assign_after, lat_at * 10, 10), limits]
    )

    def slots(first_slot, blocks):
        lasts = (low, low_left, low_right, low_far)
        return call(
            functools.partial(slot_kernel, first_slot),
            [
                jax.ShapeDtypeStruct((5, 2 * fields, 641), BF16),
                jax.ShapeDtypeStruct((32, 72, 128), BF16),
            ],
            14,
            grid_spec=pltpu.PrefetchScalarGridSpec(
                num_scalar_prefetch=1,
                grid=(5,),
                in_specs=[
                    pl.BlockSpec((1, 4, 192, 160), lambda q, *_: (q + first_slot, 0, 0, 0)),
                ]
                + [pl.BlockSpec((160, 640), lambda q, *_: (q, 0))] * 4
                + [pl.BlockSpec((32, 640), lambda q, *_: (25, 0))] * 4
                + [
                    pl.BlockSpec((1,) + t.shape[1:], lambda q, *_: (q + first_slot, 0, 0))
                    for t in turned
                ],
                out_specs=[
                    pl.BlockSpec((1, 2 * fields, 641), lambda q, *_: (q, 0, 0)),
                    pl.BlockSpec((32, 72, 128), lambda q, *_: (0, 0, 0)),
                ],
                scratch_shapes=[pltpu.VMEM((32 * 72, 128), F32)],
            ),
            name="slots",
        )(info, waves, *blocks, *lasts, *turned)

    first_rows, first_wire = slots(0, (low, low_left, low_right, low_far))
    first_wire = lax.all_to_all(first_wire, "lat", split_axis=0, concat_axis=0, tiled=True)
    later_rows, later_wire = slots(5, (high, high_left, high_right, high_far))
    later_wire = lax.all_to_all(later_wire, "lat", split_axis=0, concat_axis=0, tiled=True)

    late_half = (lat_at >= 16).astype(jnp.int32).reshape(1)
    grids = call(
        inverse_kernel,
        [
            jax.ShapeDtypeStruct((20, fields, 1280), F32),
            jax.ShapeDtypeStruct((10, fields, 640), F32),
            jax.ShapeDtypeStruct((5, fields, 320), F32),
        ],
        24,
        in_specs=[pl.BlockSpec(memory_space=pltpu.SMEM)] + [vmem] * 5,
        out_specs=[vmem] * 3,
        name="inverse",
    )(late_half, first_wire, later_wire, *tables)
    grids = [jnp.transpose(g, (1, 0, 2)) for g in grids]
    spectrum = jnp.concatenate([first_rows, later_rows], axis=0).reshape(10, 2, fields, 641)
    spectrum = jnp.transpose(spectrum, (2, 1, 0, 3))
    return (spectrum, *grids)


def solution(mesh):
    return jax.shard_map(
        on_device,
        mesh=mesh,
        in_specs=(
            P("fld", "lat", None),
            P(),
            P(),
            P("lat", None, "fld"),
            P("lat", None, None),
            P("lat", None, None),
            P("lat", None, None),
        ),
        out_specs=(
            P("fld", None, "lat", None),
            P("fld", "lat", None),
            P("fld", "lat", None),
            P("fld", "lat", None),
        ),
        check_vma=False,
    )
```

```python
import math

import jax
import jax.numpy as jnp
from jax import lax
from jax.experimental import pallas as pl
from jax.experimental.pallas import tpu as pltpu
from jax.sharding import PartitionSpec as P


F32 = jnp.float32
BF16 = jnp.bfloat16

COS_TERMS = (
    1.0,
    -4.93480110168457,
    4.058694839477539,
    -1.3351584672927856,
    0.23502981662750244,
    -0.025358986109495163,
    0.0015939108561724424,
)
SIN_TERMS = (
    3.141592502593994,
    -5.167698860168457,
    2.5499982833862305,
    -0.5985506176948547,
    0.0807478278875351,
    -0.006089475005865097,
)

NT = (((1,), (1,)), ((), ()))
NN = (((1,), (0,)), ((), ()))


def whole(shape):
    return pl.BlockSpec(shape, lambda *_: (0,) * len(shape))


def turn(count, period):
    left = count - period * jnp.floor(count * (1.0 / period) + 0.5)
    place = left * (2.0 / period)
    square = place * place
    cosine = jnp.full_like(square, COS_TERMS[-1])
    for term in COS_TERMS[-2::-1]:
        cosine = cosine * square + term
    sine = jnp.full_like(square, SIN_TERMS[-1])
    for term in SIN_TERMS[-2::-1]:
        sine = sine * square + term
    return cosine, sine * place


def fill_table(wave, shift, scale, high_cos, high_sin, table_ref, period):
    count, width = table_ref.shape
    step = 16
    many = count // step
    low = lax.broadcasted_iota(jnp.int32, (step, width), 0).astype(F32)
    low_cos, low_sin = turn(low * wave, period)
    high = lax.broadcasted_iota(jnp.int32, (many, width), 0).astype(F32)
    first, second = turn(high * (wave * float(step)) + shift, period)
    high_cos[:many, :] = first * scale
    high_sin[:many, :] = second * scale

    def body(k, carry):
        value = high_cos[pl.ds(k, 1), :] * low_cos - high_sin[pl.ds(k, 1), :] * low_sin
        table_ref[pl.ds(pl.multiple_of(k * step, step), step), :] = value.astype(BF16)
        return carry

    lax.fori_loop(0, many, body, 0)


def identity(size):
    across = lax.broadcasted_iota(jnp.int32, (size, size), 0)
    along = lax.broadcasted_iota(jnp.int32, (size, size), 1)
    return jnp.where(across == along, 1.0, 0.0).astype(BF16)


def dft_kernel(
    waves_ref,
    grid_hbm,
    wire_hbm,
    grid_ref,
    out_ref,
    even_ref,
    odd_ref,
    add_ref,
    sub_ref,
    turned_ref,
    high_cos,
    high_sin,
    in_sem,
    out_sem,
):
    half = grid_hbm.shape[1] // 2
    rows = grid_hbm.shape[0]
    incoming = pltpu.make_async_copy(grid_hbm, grid_ref, in_sem)
    incoming.start()
    lane = lax.broadcasted_iota(jnp.int32, (1, 768), 1).astype(F32)
    lane = lane - 24.0 * jnp.floor((lane + 0.5) * (1.0 / 24.0))
    size = 1.0 / math.sqrt(2 * half)
    for at, table_ref, first in ((0, even_ref, 0.0), (1, odd_ref, 4.0)):
        valid = (lane >= first) & (lane < first + 20.0)
        fill_table(
            waves_ref[at : at + 1, :],
            jnp.where(lane >= first + 10.0, half / 2.0, 0.0),
            jnp.where(valid, size, 0.0),
            high_cos,
            high_sin,
            table_ref,
            2 * half,
        )
    incoming.wait()

    def fold(k, carry):
        part = pl.ds(pl.multiple_of(k * 64, 64), 64)
        first = grid_ref[part, :half].astype(F32)
        second = grid_ref[part, half:].astype(F32)
        add_ref[part, :] = (first + second).astype(BF16)
        sub_ref[part, :] = (first - second).astype(BF16)
        return carry

    lax.fori_loop(0, rows // 64, fold, 0)
    same = identity(128)
    leaving = []
    for k in range(2):
        results = []
        for table_ref, folded_ref in ((even_ref, add_ref), (odd_ref, sub_ref)):
            for t in range(3):
                columns = slice(k * 384 + 128 * t, k * 384 + 128 * t + 128)
                turned_ref[128 * t : 128 * t + 128, :] = lax.dot_general(
                    same, table_ref[:, columns], NT, preferred_element_type=F32
                ).astype(BF16)
            results.append(
                lax.dot_general(turned_ref[...], folded_ref[...], NT, preferred_element_type=F32)
            )
        even, odd = results
        for d in range(16):
            one = even[24 * d : 24 * d + 24]
            two = odd[24 * d : 24 * d + 24]
            value = jnp.concatenate([one[:16], one[16:] + two[:8], two[8:]], axis=0)
            out_ref[k * 16 + d, :, :rows] = value.astype(BF16)
        part = pl.ds(16 * k, 16)
        leaving.append(pltpu.make_async_copy(out_ref.at[part], wire_hbm.at[part], out_sem.at[k]))
        leaving[-1].start()
    for copy in leaving:
        copy.wait()


def pack_kernel(block_ref, low_ref, high_ref, last_ref):
    step = pl.program_id(0)
    lane = lax.broadcasted_iota(jnp.int32, (160, 128), 1)
    last = jnp.zeros((160, 128), F32)
    for k in range(2):
        q = 2 * step + k
        value = block_ref[k]
        last += pltpu.roll(jnp.where(lane == 0, value[:, 640:].astype(F32), 0.0), q, 1)

        @pl.when(q < 5)
        def _():
            low_ref[pl.ds(pl.multiple_of(q * 160, 160), 160), :] = value[:, :640]

        @pl.when(q >= 5)
        def _():
            high_ref[pl.ds(pl.multiple_of(q * 160 - 800, 160), 160), :] = value[:, :640]

    @pl.when(step == 0)
    def _():
        last_ref[...] = last

    @pl.when(step > 0)
    def _():
        last_ref[...] += last

    @pl.when(step == 4)
    def _():
        for t in range(5):
            low_ref[800:832, 128 * t : 128 * t + 128] = last_ref[32 * t : 32 * t + 32, :].astype(BF16)


def lanes_kernel(wire_ref, out_ref, north_ref, south_ref):
    fields = north_ref.shape[1] // 40
    lane = lax.broadcasted_iota(jnp.int32, (40, 128), 1)

    def field(f, carry):
        base = pl.multiple_of(jnp.minimum(f * 40 // 128, 6) * 128, 128)
        offset = f * 40 - base
        rows = pl.ds(pl.multiple_of(f * 40, 8), 40)
        for half, target in ((0, north_ref), (16, south_ref)):
            rolled = {}
            for t in range(5):
                tile = None
                for k in range(128 * t // 40, min(15, (128 * t + 127) // 40) + 1):
                    if k not in rolled:
                        window = wire_ref[half + k, :, pl.ds(base, 256)]
                        shift = lax.rem(40 * k % 128 - offset + 256, 128)
                        rolled[k] = (
                            pltpu.roll(window[:, :128], shift, 1),
                            pltpu.roll(window[:, 128:], shift, 1),
                        )
                    start = 40 * k - 128 * t
                    piece = jnp.where(lane + (offset - start) >= 128, rolled[k][1], rolled[k][0])
                    tile = piece if tile is None else jnp.where(lane >= start, piece, tile)
                target[t, rows, :] = tile.astype(F32)
        return carry

    lax.fori_loop(0, fields, field, 0)

    across = lax.broadcasted_iota(jnp.int32, (128, 128), 0)
    along = lax.broadcasted_iota(jnp.int32, (128, 128), 1)
    mirror = jnp.where(across + along == 127, 1.0, 0.0).astype(BF16)

    def fold(k, carry):
        rows = pl.ds(pl.multiple_of(k * 96, 96), 96)
        south = [
            lax.dot_general(
                south_ref[4 - t, rows, :].astype(BF16), mirror, NN, preferred_element_type=F32
            )
            for t in range(5)
        ]
        for t in range(5):
            first = north_ref[t, rows, :]
            north_ref[t, rows, :] = first + south[t]
            south_ref[t, rows, :] = first - south[t]
        return carry

    lax.fori_loop(0, north_ref.shape[1] // 96, fold, 0)

    def slot(q, carry):
        for t in range(5):
            parts = [
                source[t, pl.ds(g * 10 + q, fields, stride=40), :]
                for source in (north_ref, south_ref)
                for g in range(4)
            ]
            out_ref[q, :, 128 * t : 128 * t + 128] = jnp.concatenate(parts, axis=0).astype(BF16)
        return carry

    lax.fori_loop(0, out_ref.shape[0], slot, 0)


def turn_tables_kernel(one_ref, two_ref, three_ref, out_one, out_two, out_three, *picks):
    levels = ((one_ref, out_one, 4), (two_ref, out_two, 2), (three_ref, out_three, 1))

    @pl.when(pl.program_id(0) == 0)
    def _():
        for pick_ref, (source, _, groups) in zip(picks, levels):
            size = source.shape[1]
            row = lax.broadcasted_iota(jnp.int32, (size, size), 0)
            column = lax.broadcasted_iota(jnp.int32, (size, size), 1)
            b = row // (16 * groups)
            a = (row // 16) % groups
            place = (row % 16) * (5 * groups) + 5 * a + b
            pick_ref[...] = jnp.where(place == column, 1.0, 0.0).astype(BF16)

    for pick_ref, (source, target, _) in zip(picks, levels):
        target[0] = lax.dot_general(
            pick_ref[...], source[0], NT, preferred_element_type=F32
        ).astype(BF16)


def slot_kernel(
    info_ref,
    waves_ref,
    own_low,
    left_low,
    right_low,
    far_low,
    own_high,
    left_high,
    right_high,
    far_high,
    one_ref,
    two_ref,
    three_ref,
    spectrum_hbm,
    wire_hbm,
    spectrum_ref,
    block_ref,
    last_ref,
    pack_ref,
    wire_ref,
    spectrum_sem,
    block_sem,
    last_sem,
    wire_sem,
):
    slot = pl.program_id(0)
    x = info_ref[0]
    p = info_ref[1 + slot]
    lows = (own_low, right_low, far_low, left_low)
    highs = (own_high, right_high, far_high, left_high)

    def copies(sources, q, first):
        out = []
        for step, source in enumerate(sources):
            place = pl.multiple_of(((x + step) % 4) * 160, 160)
            out.append(
                pltpu.make_async_copy(
                    source.at[pl.ds(pl.multiple_of((q - first) * 160, 160), 160), :],
                    block_ref.at[q % 2, pl.ds(place, 160), pl.ds(0, 640)],
                    block_sem.at[q % 2, step],
                )
            )
        return out

    def fetch(q):
        @pl.when(q < 5)
        def _():
            for copy in copies(lows, q, 0):
                copy.start()

        @pl.when(q >= 5)
        def _():
            for copy in copies(highs, q, 5):
                copy.start()

    @pl.when(slot == 0)
    def _():
        fetch(slot)
        lasts = [
            pltpu.make_async_copy(
                source.at[pl.ds(800, 32), :], last_ref.at[step], last_sem.at[step]
            )
            for step, source in enumerate(lows)
        ]
        for copy in lasts:
            copy.start()
        for row in range(140, 144):
            pack_ref[pl.ds(row, 32, stride=144), :] = jnp.zeros((32, 128), F32)
        for copy in lasts:
            copy.wait()
        for step in range(4):
            value = last_ref[step]
            value = jnp.concatenate([value[:, 128 * t : 128 * t + 128] for t in range(5)], axis=0)
            place = pl.multiple_of(((x + step) % 4) * 160, 160)
            for k in range(2):
                block_ref[k, pl.ds(place, 160), 640:] = value

    @pl.when(slot < 9)
    def _():
        fetch(slot + 1)

    for copy in copies(lows, slot, slot):
        copy.wait()
    total = lax.dot_general(waves_ref[0], block_ref[slot % 2], NN, preferred_element_type=F32)
    total = jnp.concatenate(
        [total[:, :640], pltpu.roll(total[:, 640:], lax.rem(128 - slot, 128), 1)], axis=1
    )
    rank = lax.broadcasted_iota(jnp.int32, (48, 768), 1)
    even_pair = p % 2 == 0
    sym = rank < 321
    place = jnp.where(sym, rank, rank - 321)
    bound = jnp.where(sym, (641 - p) // 2, (640 - p) // 2)
    first = (place < bound) == even_pair
    chosen = jnp.where(
        sym,
        jnp.where(first, total[0:48], total[48:96]),
        jnp.where(first, total[96:144], total[144:192]),
    ).astype(BF16)
    spectrum_ref[slot] = chosen[:, :641]
    pltpu.make_async_copy(
        spectrum_ref.at[slot], spectrum_hbm.at[slot], spectrum_sem.at[slot]
    ).start()
    rows = chosen.astype(F32)
    group = 0
    for level, table_ref, count in ((0, one_ref, 4), (1, two_ref, 2), (2, three_ref, 1)):
        size = table_ref.shape[1]
        half = size // 2
        limit = info_ref[11 + level]
        lane = lax.broadcasted_iota(jnp.int32, (48, size), 1)
        is_sym = lane < half
        later = pltpu.roll(rows, 768 - 321 + half, 1)[:, :size]
        order = p + jnp.where(is_sym, 2 * lane, 2 * (lane - half) + 1)
        kept = jnp.where(order <= limit, jnp.where(is_sym, rows[:, :size], later), 0.0)
        both = jnp.concatenate(
            [kept, jnp.where(is_sym, kept, -kept), jnp.zeros((32, size), F32)], axis=0
        ).astype(BF16)
        value = lax.dot_general(table_ref[0], both, NT, preferred_element_type=F32)
        many = 16 * count
        lane = lax.broadcasted_iota(jnp.int32, (many, 128), 1)
        for sign in range(2):
            for c in range(2):
                packed = jnp.zeros((many, 128), F32)
                for b in range(5):
                    part = value[many * b : many * b + many]
                    move = 24 * (b - 2 * sign - c) % 128
                    if move:
                        part = pltpu.roll(part, move, 1)
                    packed = jnp.where((lane >= 24 * b) & (lane < 24 * b + 24), part, packed)
                for a in range(count):
                    start = sign * 16 * 144 + 20 * (group + a) + 10 * c + slot
                    pack_ref[pl.ds(start, 16, stride=144), :] = packed[16 * a : 16 * a + 16]
        group += count

    @pl.when(slot == pl.num_programs(0) - 1)
    def _():
        for d in range(16):
            wire_ref[d] = pack_ref[144 * d : 144 * d + 144, :].astype(BF16)
            wire_ref[31 - d] = pack_ref[144 * (16 + d) : 144 * (17 + d), :].astype(BF16)
        leaving = pltpu.make_async_copy(wire_ref, wire_hbm, wire_sem)
        leaving.start()
        for k in range(10):
            pltpu.make_async_copy(
                spectrum_ref.at[k], spectrum_hbm.at[k], spectrum_sem.at[k]
            ).wait()
        leaving.wait()


def inverse_table_kernel(waves_ref, table_ref, high_cos, high_sin):
    wave = waves_ref[0:1, :]
    lane = lax.broadcasted_iota(jnp.int32, (1, 768), 1).astype(F32)
    lane = lane - 24.0 * jnp.floor((lane + 0.5) * (1.0 / 24.0))
    weight = jnp.where(lane < 20.0, jnp.where(wave == 0.0, 1.0, 2.0), 0.0)
    first = 0
    for period in (1280, 640, 320):
        shift = jnp.where(lane >= 10.0, period / 4.0, 0.0)
        scale = weight * (1.0 / math.sqrt(period))
        part = table_ref.at[pl.ds(first, period), :]
        fill_table(wave, shift, scale, high_cos, high_sin, part, period)
        first += period


def inverse_kernel(
    info_ref,
    wire_ref,
    table_ref,
    out_one,
    out_two,
    out_three,
    big_ref,
    mid_ref,
    small_ref,
    out_sem,
):
    late_half = info_ref[0]
    same = identity(128)

    def lines(group):
        start = 20 * group // 8 * 8
        part = wire_ref[:, start : start + 24, :].astype(F32)
        if 20 * group > start:
            part = pltpu.roll(part, 24 - (20 * group - start), 1)
        part = part.reshape(part.shape[0] * 24, 128).astype(BF16)
        return lax.dot_general(same, part, NT, preferred_element_type=F32).astype(BF16)

    def place(target, value, count, last):
        for a in range(count):
            for b in range(5):
                row = 5 * a + b
                row = jnp.where(late_half == 1, last - row, row)
                target[row] = value[128 * a + 24 * b : 128 * a + 24 * b + 24]

    leaving = []

    def leave(source, target):
        copy = pltpu.make_async_copy(source, target, out_sem.at[len(leaving)])
        copy.start()
        leaving.append(copy)

    left = [lines(group) for group in range(7)]
    value = lax.dot_general(left[6], table_ref[1920:, :], NT, preferred_element_type=F32)
    place(small_ref, value, 1, 4)
    leave(small_ref, out_three)
    value = lax.dot_general(
        jnp.concatenate(left[4:6], axis=0),
        table_ref[1280:1920, :],
        NT,
        preferred_element_type=F32,
    )
    place(mid_ref, value, 2, 9)
    leave(mid_ref, out_two)
    left = jnp.concatenate(left[:4], axis=0)
    for n in range(5):
        columns = slice(256 * n, 256 * n + 256)
        value = lax.dot_general(left, table_ref[columns, :], NT, preferred_element_type=F32)
        place(big_ref.at[n], value, 4, 19)
        leave(big_ref.at[n], out_one.at[:, :, pl.ds(256 * n, 256)])
    for copy in leaving:
        copy.wait()


def call(kernel, out_shape, limit, **kw):
    return pl.pallas_call(
        kernel,
        out_shape=out_shape,
        compiler_params=pltpu.CompilerParams(vmem_limit_bytes=limit * 1024 * 1024),
        **kw,
    )


def on_device(grid_fields, assign, limits, legendre, synth_one, synth_two, synth_three):
    fields, rows, lon = grid_fields.shape
    lat_at = lax.axis_index("lat")
    fld_at = lax.axis_index("fld")
    vmem = pl.BlockSpec(memory_space=pltpu.VMEM)

    hbm = pl.BlockSpec(memory_space=pltpu.HBM)
    own = jnp.transpose(legendre, (0, 2, 1))
    low, high = call(
        pack_kernel,
        [jax.ShapeDtypeStruct((832, 640), BF16), jax.ShapeDtypeStruct((800, 640), BF16)],
        60,
        grid=(5,),
        in_specs=[pl.BlockSpec((2, 160, 641), lambda q: (q, 0, 0))],
        out_specs=[whole((832, 640)), whole((800, 640))],
        scratch_shapes=[pltpu.VMEM((160, 128), F32)],
        name="pack",
    )(own)
    low, high, grid_fields, assign = lax.optimization_barrier((low, high, grid_fields, assign))
    right = [(k, (k + 1) % 4) for k in range(4)]
    left = [(k, (k + 3) % 4) for k in range(4)]
    low_left = lax.ppermute(low, "fld", right)
    high_right = lax.ppermute(high, "fld", left)
    low_right = lax.ppermute(low, "fld", left)
    high_left = lax.ppermute(high, "fld", right)
    low_far = lax.ppermute(low_left, "fld", right)
    high_far = lax.ppermute(high_right, "fld", left)

    pairs = assign.reshape(32, 10)
    even = jnp.where(pairs % 2 == 0, pairs, 639 - pairs).astype(F32)
    odd = 639.0 - even
    spare = jnp.zeros((32, 4), F32)
    forward_waves = jnp.stack(
        [
            jnp.concatenate([even, even, spare], axis=1),
            jnp.concatenate([spare, odd, odd], axis=1),
        ]
    ).reshape(2, 768)
    wire = call(
        dft_kernel,
        jax.ShapeDtypeStruct((32, 40, 1024), BF16),
        60,
        in_specs=[vmem, hbm],
        out_specs=hbm,
        scratch_shapes=[
            pltpu.VMEM((fields * rows, lon), BF16),
            pltpu.VMEM((32, 40, 1024), BF16),
            pltpu.VMEM((lon // 2, 768), BF16),
            pltpu.VMEM((lon // 2, 768), BF16),
            pltpu.VMEM((fields * rows, lon // 2), BF16),
            pltpu.VMEM((fields * rows, lon // 2), BF16),
            pltpu.VMEM((384, lon // 2), BF16),
            pltpu.VMEM((80, 768), F32),
            pltpu.VMEM((80, 768), F32),
            pltpu.SemaphoreType.DMA(()),
            pltpu.SemaphoreType.DMA((2,)),
        ],
        name="dft",
    )(forward_waves, grid_fields.reshape(fields * rows, lon))
    assign_after, synth_one, synth_two, synth_three, wire = lax.optimization_barrier(
        (assign, synth_one, synth_two, synth_three, wire)
    )
    wire = lax.all_to_all(wire, "lat", split_axis=0, concat_axis=0, tiled=True)

    synths = (synth_one, synth_two, synth_three)
    slot_block = [pl.BlockSpec((1,) + t.shape[1:], lambda q: (q, 0, 0)) for t in synths]
    turned = call(
        turn_tables_kernel,
        [jax.ShapeDtypeStruct(t.shape, BF16) for t in synths],
        60,
        grid=(10,),
        in_specs=slot_block,
        out_specs=slot_block,
        scratch_shapes=[pltpu.VMEM(t.shape[1:], BF16) for t in synths],
        name="turn_tables",
    )(*synths)

    plain = assign_after.reshape(32, 10).astype(F32)
    spare = jnp.zeros((32, 4), F32)
    inverse_waves = jnp.concatenate([plain, plain, spare], axis=1).reshape(1, 768)
    table = call(
        inverse_table_kernel,
        jax.ShapeDtypeStruct((2240, 768), BF16),
        12,
        in_specs=[vmem],
        out_specs=vmem,
        scratch_shapes=[pltpu.VMEM((80, 768), F32), pltpu.VMEM((80, 768), F32)],
        name="inverse_tables",
    )(inverse_waves)

    waves = call(
        lanes_kernel,
        jax.ShapeDtypeStruct((10, 192, 640), BF16),
        18,
        in_specs=[vmem],
        out_specs=vmem,
        scratch_shapes=[
            pltpu.VMEM((5, fields * rows, 128), F32),
            pltpu.VMEM((5, fields * rows, 128), F32),
        ],
        name="lanes",
    )(wire)

    info = jnp.concatenate(
        [fld_at.reshape(1), lax.dynamic_slice_in_dim(assign_after, lat_at * 10, 10), limits]
    )
    spectrum, level_wire = call(
        slot_kernel,
        [
            jax.ShapeDtypeStruct((10, 2 * fields, 641), BF16),
            jax.ShapeDtypeStruct((32, 144, 128), BF16),
        ],
        18,
        grid_spec=pltpu.PrefetchScalarGridSpec(
            num_scalar_prefetch=1,
            grid=(10,),
            in_specs=[pl.BlockSpec((1, 192, 640), lambda q, *_: (q, 0, 0))]
            + [hbm] * 8
            + [pl.BlockSpec((1,) + t.shape[1:], lambda q, *_: (q, 0, 0)) for t in turned],
            out_specs=[hbm, hbm],
            scratch_shapes=[
                pltpu.VMEM((10, 2 * fields, 641), BF16),
                pltpu.VMEM((2, 640, 768), BF16),
                pltpu.VMEM((4, 32, 640), BF16),
                pltpu.VMEM((32 * 144, 128), F32),
                pltpu.VMEM((32, 144, 128), BF16),
                pltpu.SemaphoreType.DMA((10,)),
                pltpu.SemaphoreType.DMA((2, 4)),
                pltpu.SemaphoreType.DMA((4,)),
                pltpu.SemaphoreType.DMA(()),
            ],
        ),
        name="slots",
    )(
        info,
        waves,
        low,
        low_left,
        low_right,
        low_far,
        high,
        high_left,
        high_right,
        high_far,
        *turned,
    )
    level_wire = lax.all_to_all(level_wire, "lat", split_axis=0, concat_axis=0, tiled=True)

    late_half = (lat_at >= 16).astype(jnp.int32).reshape(1)
    grids = call(
        inverse_kernel,
        [
            jax.ShapeDtypeStruct((20, fields, 1280), F32),
            jax.ShapeDtypeStruct((10, fields, 640), F32),
            jax.ShapeDtypeStruct((5, fields, 320), F32),
        ],
        24,
        in_specs=[pl.BlockSpec(memory_space=pltpu.SMEM), vmem, vmem],
        out_specs=[hbm] * 3,
        scratch_shapes=[
            pltpu.VMEM((5, 20, fields, 256), F32),
            pltpu.VMEM((10, fields, 640), F32),
            pltpu.VMEM((5, fields, 320), F32),
            pltpu.SemaphoreType.DMA((7,)),
        ],
        name="inverse",
    )(late_half, level_wire, table)
    grids = [jnp.transpose(g, (1, 0, 2)) for g in grids]
    spectrum = jnp.transpose(spectrum.reshape(10, 2, fields, 641), (2, 1, 0, 3))
    return (spectrum, *grids)


def solution(mesh):
    return jax.shard_map(
        on_device,
        mesh=mesh,
        in_specs=(
            P("fld", "lat", None),
            P(),
            P(),
            P("lat", None, "fld"),
            P("lat", None, None),
            P("lat", None, None),
            P("lat", None, None),
        ),
        out_specs=(
            P("fld", None, "lat", None),
            P("fld", "lat", None),
            P("fld", "lat", None),
            P("fld", "lat", None),
        ),
        check_vma=False,
    )
```

```python
import math

import jax
import jax.numpy as jnp
from jax import lax
from jax.experimental import pallas as pl
from jax.experimental.pallas import tpu as pltpu
from jax.sharding import PartitionSpec as P


F32 = jnp.float32
BF16 = jnp.bfloat16

COS_TERMS = (
    1.0,
    -4.93480110168457,
    4.058694839477539,
    -1.3351584672927856,
    0.23502981662750244,
    -0.025358986109495163,
    0.0015939108561724424,
)
SIN_TERMS = (
    3.141592502593994,
    -5.167698860168457,
    2.5499982833862305,
    -0.5985506176948547,
    0.0807478278875351,
    -0.006089475005865097,
)

NT = (((1,), (1,)), ((), ()))
NN = (((1,), (0,)), ((), ()))


def turn(count, period):
    left = count - period * jnp.floor(count * (1.0 / period) + 0.5)
    place = left * (2.0 / period)
    square = place * place
    cosine = jnp.full_like(square, COS_TERMS[-1])
    for term in COS_TERMS[-2::-1]:
        cosine = cosine * square + term
    sine = jnp.full_like(square, SIN_TERMS[-1])
    for term in SIN_TERMS[-2::-1]:
        sine = sine * square + term
    return cosine, sine * place


def fill_table(wave, shift, scale, high_cos, high_sin, table_ref, period):
    count, width = table_ref.shape
    step = 16
    many = count // step
    low = lax.broadcasted_iota(jnp.int32, (step, width), 0).astype(F32)
    low_cos, low_sin = turn(low * wave, period)
    high = lax.broadcasted_iota(jnp.int32, (many, width), 0).astype(F32)
    first, second = turn(high * (wave * float(step)) + shift, period)
    high_cos[:many, :] = first * scale
    high_sin[:many, :] = second * scale

    def body(k, carry):
        value = high_cos[pl.ds(k, 1), :] * low_cos - high_sin[pl.ds(k, 1), :] * low_sin
        table_ref[pl.ds(pl.multiple_of(k * step, step), step), :] = value.astype(BF16)
        return carry

    lax.fori_loop(0, many, body, 0, unroll=4)


def identity(size):
    across = lax.broadcasted_iota(jnp.int32, (size, size), 0)
    along = lax.broadcasted_iota(jnp.int32, (size, size), 1)
    return jnp.where(across == along, 1.0, 0.0).astype(BF16)


def dft_kernel(
    info_ref,
    waves_ref,
    grid_hbm,
    wire_hbm,
    grid_ref,
    out_ref,
    even_ref,
    odd_ref,
    add_ref,
    sub_ref,
    turned_ref,
    high_cos,
    high_sin,
    in_sem,
    out_sem,
):
    half = grid_hbm.shape[1] // 2
    rows = grid_hbm.shape[0]
    incoming = pltpu.make_async_copy(grid_hbm, grid_ref, in_sem)
    incoming.start()
    lane = lax.broadcasted_iota(jnp.int32, (1, 768), 1).astype(F32)
    lane = lane - 24.0 * jnp.floor((lane + 0.5) * (1.0 / 24.0))
    size = 1.0 / math.sqrt(2 * half)
    for at, table_ref, first in ((0, even_ref, 0.0), (1, odd_ref, 4.0)):
        valid = (lane >= first) & (lane < first + 20.0)
        fill_table(
            waves_ref[at : at + 1, :],
            jnp.where(lane >= first + 10.0, half / 2.0, 0.0),
            jnp.where(valid, size, 0.0),
            high_cos,
            high_sin,
            table_ref,
            2 * half,
        )
    incoming.wait()

    def fold(k, carry):
        part = pl.ds(pl.multiple_of(k * 64, 64), 64)
        first = grid_ref[part, :half].astype(F32)
        second = grid_ref[part, half:].astype(F32)
        add_ref[part, :] = (first + second).astype(BF16)
        sub_ref[part, :] = (first - second).astype(BF16)
        return carry

    lax.fori_loop(0, rows // 64, fold, 0)
    add_ref[rows:, :] = jnp.zeros((1024 - rows, half), BF16)
    sub_ref[rows:, :] = jnp.zeros((1024 - rows, half), BF16)
    same = identity(128)
    turn_by = info_ref[0]
    shift = lax.rem(turn_by, 128)
    tile_shift = lax.div(turn_by, 128)
    lane = lax.broadcasted_iota(jnp.int32, (40, 128), 1)
    leaving = []
    for k in range(2):
        results = []
        for table_ref, folded_ref in ((even_ref, add_ref), (odd_ref, sub_ref)):
            for t in range(3):
                columns = slice(k * 384 + 128 * t, k * 384 + 128 * t + 128)
                turned_ref[128 * t : 128 * t + 128, :] = lax.dot_general(
                    same, table_ref[:, columns], NT, preferred_element_type=F32
                ).astype(BF16)
            results.append(
                lax.dot_general(turned_ref[...], folded_ref[...], NT, preferred_element_type=F32)
            )
        even, odd = results
        for d in range(16):
            one = even[24 * d : 24 * d + 24]
            two = odd[24 * d : 24 * d + 24]
            value = jnp.concatenate([one[:16], one[16:] + two[:8], two[8:]], axis=0)
            tiles = [pltpu.roll(value[:, 128 * t : 128 * t + 128], shift, 1) for t in range(8)]
            for t in range(8):
                tile = jnp.where(lane < shift, tiles[t - 1], tiles[t])
                place = pl.multiple_of(lax.rem(tile_shift + t, 8) * 128, 128)
                out_ref[k * 16 + d, :, pl.ds(place, 128)] = tile.astype(BF16)
        part = pl.ds(16 * k, 16)
        leaving.append(pltpu.make_async_copy(out_ref.at[part], wire_hbm.at[part], out_sem.at[k]))
        leaving[-1].start()
    for copy in leaving:
        copy.wait()


def pack_kernel(block_hbm, low_hbm, high_hbm, low_ref, high_ref, edge_ref, in_sem, out_sem):
    edge = pltpu.make_async_copy(block_hbm.at[:, :, pl.ds(640, 1)], edge_ref, in_sem.at[10])
    edge.start()
    incoming = []
    for q in range(10):
        target = low_ref if q < 5 else high_ref
        incoming.append(
            pltpu.make_async_copy(
                block_hbm.at[q, :, pl.ds(0, 640)],
                target.at[pl.ds(q % 5 * 160, 160), :],
                in_sem.at[q],
            )
        )
        incoming[-1].start()
    edge.wait()
    lane = lax.broadcasted_iota(jnp.int32, (160, 128), 1)
    last = jnp.zeros((160, 128), F32)
    for q in range(10):
        last = jnp.where(lane == q, edge_ref[q].astype(F32), last)
    for t in range(5):
        low_ref[800:832, 128 * t : 128 * t + 128] = last[32 * t : 32 * t + 32].astype(BF16)
    for copy in incoming[:5]:
        copy.wait()
    low_out = pltpu.make_async_copy(low_ref, low_hbm, out_sem.at[0])
    low_out.start()
    for copy in incoming[5:]:
        copy.wait()
    high_out = pltpu.make_async_copy(high_ref, high_hbm, out_sem.at[1])
    high_out.start()
    low_out.wait()
    high_out.wait()


def lanes_kernel(wire_ref, out_ref, north_ref, south_ref):
    fields = north_ref.shape[1] // 40
    lane = lax.broadcasted_iota(jnp.int32, (40, 128), 1)
    for f in range(fields):
        offset = 40 * f % 128
        for half, target in ((0, north_ref), (16, south_ref)):
            tiles = []
            for o in range(6 if offset else 5):
                at = (40 * f // 128 + o) % 8 * 128
                first = 128 * o - offset
                tile = None
                for k in range(max(first // 40, 0), min((first + 127) // 40, 15) + 1):
                    piece = wire_ref[half + k, :, at : at + 128]
                    tile = piece if tile is None else jnp.where(lane >= 40 * k - first, piece, tile)
                tiles.append(tile.astype(F32))
            if offset:
                tiles = [pltpu.roll(tile, 128 - offset, 1) for tile in tiles]
                tiles = [
                    jnp.where(lane < 128 - offset, tiles[t], tiles[t + 1]) for t in range(5)
                ]
            for t in range(5):
                target[t, 40 * f : 40 * f + 40, :] = tiles[t]

    across = lax.broadcasted_iota(jnp.int32, (128, 128), 0)
    along = lax.broadcasted_iota(jnp.int32, (128, 128), 1)
    mirror = jnp.where(across + along == 127, 1.0, 0.0).astype(BF16)

    def fold(k, carry):
        rows = pl.ds(pl.multiple_of(k * 96, 96), 96)
        south = [
            lax.dot_general(
                south_ref[4 - t, rows, :].astype(BF16), mirror, NN, preferred_element_type=F32
            )
            for t in range(5)
        ]
        for t in range(5):
            first = north_ref[t, rows, :]
            north_ref[t, rows, :] = first + south[t]
            south_ref[t, rows, :] = first - south[t]
        return carry

    lax.fori_loop(0, north_ref.shape[1] // 96, fold, 0)

    def slot(q, carry):
        for t in range(5):
            parts = [
                source[t, pl.ds(g * 10 + q, fields, stride=40), :]
                for source in (north_ref, south_ref)
                for g in range(4)
            ]
            out_ref[q, :, 128 * t : 128 * t + 128] = jnp.concatenate(parts, axis=0).astype(BF16)
        return carry

    lax.fori_loop(0, out_ref.shape[0], slot, 0)


def turn_tables_kernel(one_ref, two_ref, three_ref, out_one, out_two, out_three, *picks):
    levels = ((one_ref, out_one, 4), (two_ref, out_two, 2), (three_ref, out_three, 1))

    @pl.when(pl.program_id(0) == 0)
    def _():
        for pick_ref, (source, _, groups) in zip(picks, levels):
            size = source.shape[1]
            row = lax.broadcasted_iota(jnp.int32, (size, size), 0)
            column = lax.broadcasted_iota(jnp.int32, (size, size), 1)
            b = row // (16 * groups)
            a = (row // 16) % groups
            place = (row % 16) * (5 * groups) + 5 * a + b
            pick_ref[...] = jnp.where(place == column, 1.0, 0.0).astype(BF16)

    for pick_ref, (source, target, _) in zip(picks, levels):
        target[0] = lax.dot_general(
            pick_ref[...], source[0], NT, preferred_element_type=F32
        ).astype(BF16)


def slot_kernel(
    info_ref,
    waves_ref,
    own_low,
    left_low,
    right_low,
    far_low,
    own_high,
    left_high,
    right_high,
    far_high,
    one_ref,
    two_ref,
    three_ref,
    spectrum_hbm,
    wire_hbm,
    spectrum_ref,
    block_ref,
    last_ref,
    pack_ref,
    wire_ref,
    spectrum_sem,
    block_sem,
    last_sem,
    wire_sem,
):
    slot = pl.program_id(0)
    x = info_ref[0]
    p = info_ref[1 + slot]
    lows = (own_low, right_low, far_low, left_low)
    highs = (own_high, right_high, far_high, left_high)

    def copies(sources, q, first):
        out = []
        for step, source in enumerate(sources):
            place = pl.multiple_of(((x + step) % 4) * 160, 160)
            out.append(
                pltpu.make_async_copy(
                    source.at[pl.ds(pl.multiple_of((q - first) * 160, 160), 160), :],
                    block_ref.at[q % 2, pl.ds(place, 160), pl.ds(0, 640)],
                    block_sem.at[q % 2, step],
                )
            )
        return out

    def fetch(q):
        @pl.when(q < 5)
        def _():
            for copy in copies(lows, q, 0):
                copy.start()

        @pl.when(q >= 5)
        def _():
            for copy in copies(highs, q, 5):
                copy.start()

    @pl.when(slot == 0)
    def _():
        fetch(slot)
        lasts = [
            pltpu.make_async_copy(
                source.at[pl.ds(800, 32), :], last_ref.at[step], last_sem.at[step]
            )
            for step, source in enumerate(lows)
        ]
        for copy in lasts:
            copy.start()
        for row in range(140, 144):
            pack_ref[pl.ds(row, 32, stride=144), :] = jnp.zeros((32, 128), F32)
        for copy in lasts:
            copy.wait()
        for step in range(4):
            value = last_ref[step]
            value = jnp.concatenate([value[:, 128 * t : 128 * t + 128] for t in range(5)], axis=0)
            place = pl.multiple_of(((x + step) % 4) * 160, 160)
            for k in range(2):
                block_ref[k, pl.ds(place, 160), 640:] = value

    @pl.when(slot < 9)
    def _():
        fetch(slot + 1)

    for copy in copies(lows, slot, slot):
        copy.wait()
    total = lax.dot_general(waves_ref[0], block_ref[slot % 2], NN, preferred_element_type=F32)
    total = jnp.concatenate(
        [total[:, :640], pltpu.roll(total[:, 640:], lax.rem(128 - slot, 128), 1)], axis=1
    )
    rank = lax.broadcasted_iota(jnp.int32, (48, 768), 1)
    even_pair = p % 2 == 0
    sym = rank < 321
    place = jnp.where(sym, rank, rank - 321)
    bound = jnp.where(sym, (641 - p) // 2, (640 - p) // 2)
    first = (place < bound) == even_pair
    chosen = jnp.where(
        sym,
        jnp.where(first, total[0:48], total[48:96]),
        jnp.where(first, total[96:144], total[144:192]),
    ).astype(BF16)
    spectrum_ref[slot] = chosen[:, :641]
    pltpu.make_async_copy(
        spectrum_ref.at[slot], spectrum_hbm.at[slot], spectrum_sem.at[slot]
    ).start()
    rows = chosen.astype(F32)
    group = 0
    for level, table_ref, count in ((0, one_ref, 4), (1, two_ref, 2), (2, three_ref, 1)):
        size = table_ref.shape[1]
        half = size // 2
        limit = info_ref[11 + level]
        lane = lax.broadcasted_iota(jnp.int32, (48, size), 1)
        is_sym = lane < half
        later = pltpu.roll(rows, 768 - 321 + half, 1)[:, :size]
        order = p + jnp.where(is_sym, 2 * lane, 2 * (lane - half) + 1)
        kept = jnp.where(order <= limit, jnp.where(is_sym, rows[:, :size], later), 0.0)
        both = jnp.concatenate(
            [kept, jnp.where(is_sym, kept, -kept), jnp.zeros((32, size), F32)], axis=0
        ).astype(BF16)
        value = lax.dot_general(table_ref[0], both, NT, preferred_element_type=F32)
        many = 16 * count
        lane = lax.broadcasted_iota(jnp.int32, (many, 128), 1)
        for sign in range(2):
            for c in range(2):
                packed = jnp.zeros((many, 128), F32)
                for b in range(5):
                    part = value[many * b : many * b + many]
                    move = 24 * (b - 2 * sign - c) % 128
                    if move:
                        part = pltpu.roll(part, move, 1)
                    packed = jnp.where((lane >= 24 * b) & (lane < 24 * b + 24), part, packed)
                for a in range(count):
                    start = sign * 16 * 144 + 20 * (group + a) + 10 * c + slot
                    pack_ref[pl.ds(start, 16, stride=144), :] = packed[16 * a : 16 * a + 16]
        group += count

    @pl.when(slot == pl.num_programs(0) - 1)
    def _():
        for d in range(16):
            wire_ref[d] = pack_ref[144 * d : 144 * d + 144, :].astype(BF16)
            wire_ref[31 - d] = pack_ref[144 * (16 + d) : 144 * (17 + d), :].astype(BF16)
        leaving = pltpu.make_async_copy(wire_ref, wire_hbm, wire_sem)
        leaving.start()
        for k in range(10):
            pltpu.make_async_copy(
                spectrum_ref.at[k], spectrum_hbm.at[k], spectrum_sem.at[k]
            ).wait()
        leaving.wait()


def inverse_table_kernel(waves_ref, table_ref, high_cos, high_sin):
    wave = waves_ref[0:1, :]
    lane = lax.broadcasted_iota(jnp.int32, (1, 768), 1).astype(F32)
    lane = lane - 24.0 * jnp.floor((lane + 0.5) * (1.0 / 24.0))
    weight = jnp.where(lane < 20.0, jnp.where(wave == 0.0, 1.0, 2.0), 0.0)
    first = 0
    for period in (1280, 640, 320):
        shift = jnp.where(lane >= 10.0, period / 4.0, 0.0)
        scale = weight * (1.0 / math.sqrt(period))
        part = table_ref.at[pl.ds(first, period), :]
        fill_table(wave, shift, scale, high_cos, high_sin, part, period)
        first += period


def inverse_kernel(
    info_ref,
    wire_ref,
    table_ref,
    out_one,
    out_two,
    out_three,
    big_ref,
    mid_ref,
    small_ref,
    out_sem,
):
    late_half = info_ref[0]
    same = identity(128)

    def lines(group):
        start = 20 * group // 8 * 8
        part = wire_ref[:, start : start + 24, :].astype(F32)
        if 20 * group > start:
            part = pltpu.roll(part, 24 - (20 * group - start), 1)
        part = part.reshape(part.shape[0] * 24, 128).astype(BF16)
        return lax.dot_general(same, part, NT, preferred_element_type=F32).astype(BF16)

    def place(target, value, count, last):
        for a in range(count):
            for b in range(5):
                row = 5 * a + b
                row = jnp.where(late_half == 1, last - row, row)
                target[row] = value[128 * a + 24 * b : 128 * a + 24 * b + 24]

    leaving = []

    def leave(source, target):
        copy = pltpu.make_async_copy(source, target, out_sem.at[len(leaving)])
        copy.start()
        leaving.append(copy)

    left = [lines(group) for group in range(7)]
    value = lax.dot_general(left[6], table_ref[1920:, :], NT, preferred_element_type=F32)
    place(small_ref, value, 1, 4)
    leave(small_ref, out_three)
    value = lax.dot_general(
        jnp.concatenate(left[4:6], axis=0),
        table_ref[1280:1920, :],
        NT,
        preferred_element_type=F32,
    )
    place(mid_ref, value, 2, 9)
    leave(mid_ref, out_two)
    left = jnp.concatenate(left[:4], axis=0)
    for n in range(5):
        columns = slice(256 * n, 256 * n + 256)
        value = lax.dot_general(left, table_ref[columns, :], NT, preferred_element_type=F32)
        place(big_ref.at[n], value, 4, 19)
        leave(big_ref.at[n], out_one.at[:, :, pl.ds(256 * n, 256)])
    for copy in leaving:
        copy.wait()


def call(kernel, out_shape, limit, **kw):
    return pl.pallas_call(
        kernel,
        out_shape=out_shape,
        compiler_params=pltpu.CompilerParams(vmem_limit_bytes=limit * 1024 * 1024),
        **kw,
    )


def on_device(grid_fields, assign, limits, legendre, synth_one, synth_two, synth_three):
    fields, rows, lon = grid_fields.shape
    lat_at = lax.axis_index("lat")
    fld_at = lax.axis_index("fld")
    vmem = pl.BlockSpec(memory_space=pltpu.VMEM)

    hbm = pl.BlockSpec(memory_space=pltpu.HBM)
    own = jnp.transpose(legendre, (0, 2, 1))
    low, high = call(
        pack_kernel,
        [jax.ShapeDtypeStruct((832, 640), BF16), jax.ShapeDtypeStruct((800, 640), BF16)],
        60,
        in_specs=[hbm],
        out_specs=[hbm, hbm],
        scratch_shapes=[
            pltpu.VMEM((832, 640), BF16),
            pltpu.VMEM((800, 640), BF16),
            pltpu.VMEM((10, 160, 1), BF16),
            pltpu.SemaphoreType.DMA((11,)),
            pltpu.SemaphoreType.DMA((2,)),
        ],
        name="pack",
    )(own)
    low, high, grid_fields, assign = lax.optimization_barrier((low, high, grid_fields, assign))
    right = [(k, (k + 1) % 4) for k in range(4)]
    left = [(k, (k + 3) % 4) for k in range(4)]
    low_left = lax.ppermute(low, "fld", right)
    high_right = lax.ppermute(high, "fld", left)
    low_right = lax.ppermute(low, "fld", left)
    high_left = lax.ppermute(high, "fld", right)
    low_far = lax.ppermute(low_left, "fld", right)
    high_far = lax.ppermute(high_right, "fld", left)

    pairs = assign.reshape(32, 10)
    even = jnp.where(pairs % 2 == 0, pairs, 639 - pairs).astype(F32)
    odd = 639.0 - even
    spare = jnp.zeros((32, 4), F32)
    forward_waves = jnp.stack(
        [
            jnp.concatenate([even, even, spare], axis=1),
            jnp.concatenate([spare, odd, odd], axis=1),
        ]
    ).reshape(2, 768)
    wire = call(
        dft_kernel,
        jax.ShapeDtypeStruct((32, 40, 1024), BF16),
        60,
        in_specs=[pl.BlockSpec(memory_space=pltpu.SMEM), vmem, hbm],
        out_specs=hbm,
        scratch_shapes=[
            pltpu.VMEM((fields * rows, lon), BF16),
            pltpu.VMEM((32, 40, 1024), BF16),
            pltpu.VMEM((lon // 2, 768), BF16),
            pltpu.VMEM((lon // 2, 768), BF16),
            pltpu.VMEM((1024, lon // 2), BF16),
            pltpu.VMEM((1024, lon // 2), BF16),
            pltpu.VMEM((384, lon // 2), BF16),
            pltpu.VMEM((80, 768), F32),
            pltpu.VMEM((80, 768), F32),
            pltpu.SemaphoreType.DMA(()),
            pltpu.SemaphoreType.DMA((2,)),
        ],
        name="dft",
    )((lat_at % 16 * 40).reshape(1), forward_waves, grid_fields.reshape(fields * rows, lon))
    assign_after, synth_one, synth_two, synth_three, wire = lax.optimization_barrier(
        (assign, synth_one, synth_two, synth_three, wire)
    )
    wire = lax.all_to_all(wire, "lat", split_axis=0, concat_axis=0, tiled=True)

    synths = (synth_one, synth_two, synth_three)
    slot_block = [pl.BlockSpec((1,) + t.shape[1:], lambda q: (q, 0, 0)) for t in synths]
    turned = call(
        turn_tables_kernel,
        [jax.ShapeDtypeStruct(t.shape, BF16) for t in synths],
        60,
        grid=(10,),
        in_specs=slot_block,
        out_specs=slot_block,
        scratch_shapes=[pltpu.VMEM(t.shape[1:], BF16) for t in synths],
        name="turn_tables",
    )(*synths)

    plain = assign_after.reshape(32, 10).astype(F32)
    spare = jnp.zeros((32, 4), F32)
    inverse_waves = jnp.concatenate([plain, plain, spare], axis=1).reshape(1, 768)
    table = call(
        inverse_table_kernel,
        jax.ShapeDtypeStruct((2240, 768), BF16),
        12,
        in_specs=[vmem],
        out_specs=vmem,
        scratch_shapes=[pltpu.VMEM((80, 768), F32), pltpu.VMEM((80, 768), F32)],
        name="inverse_tables",
    )(inverse_waves)

    waves = call(
        lanes_kernel,
        jax.ShapeDtypeStruct((10, 192, 640), BF16),
        18,
        in_specs=[vmem],
        out_specs=vmem,
        scratch_shapes=[
            pltpu.VMEM((5, fields * rows, 128), F32),
            pltpu.VMEM((5, fields * rows, 128), F32),
        ],
        name="lanes",
    )(wire)

    info = jnp.concatenate(
        [fld_at.reshape(1), lax.dynamic_slice_in_dim(assign_after, lat_at * 10, 10), limits]
    )
    spectrum, level_wire = call(
        slot_kernel,
        [
            jax.ShapeDtypeStruct((10, 2 * fields, 641), BF16),
            jax.ShapeDtypeStruct((32, 144, 128), BF16),
        ],
        60,
        grid_spec=pltpu.PrefetchScalarGridSpec(
            num_scalar_prefetch=1,
            grid=(10,),
            in_specs=[pl.BlockSpec((1, 192, 640), lambda q, *_: (q, 0, 0))]
            + [hbm] * 8
            + [pl.BlockSpec((1,) + t.shape[1:], lambda q, *_: (q, 0, 0)) for t in turned],
            out_specs=[hbm, hbm],
            scratch_shapes=[
                pltpu.VMEM((10, 2 * fields, 641), BF16),
                pltpu.VMEM((2, 640, 768), BF16),
                pltpu.VMEM((4, 32, 640), BF16),
                pltpu.VMEM((32 * 144, 128), F32),
                pltpu.VMEM((32, 144, 128), BF16),
                pltpu.SemaphoreType.DMA((10,)),
                pltpu.SemaphoreType.DMA((2, 4)),
                pltpu.SemaphoreType.DMA((4,)),
                pltpu.SemaphoreType.DMA(()),
            ],
        ),
        name="slots",
    )(
        info,
        waves,
        low,
        low_left,
        low_right,
        low_far,
        high,
        high_left,
        high_right,
        high_far,
        *turned,
    )
    level_wire = lax.all_to_all(level_wire, "lat", split_axis=0, concat_axis=0, tiled=True)

    late_half = (lat_at >= 16).astype(jnp.int32).reshape(1)
    grids = call(
        inverse_kernel,
        [
            jax.ShapeDtypeStruct((20, fields, 1280), F32),
            jax.ShapeDtypeStruct((10, fields, 640), F32),
            jax.ShapeDtypeStruct((5, fields, 320), F32),
        ],
        24,
        in_specs=[pl.BlockSpec(memory_space=pltpu.SMEM), vmem, vmem],
        out_specs=[hbm] * 3,
        scratch_shapes=[
            pltpu.VMEM((5, 20, fields, 256), F32),
            pltpu.VMEM((10, fields, 640), F32),
            pltpu.VMEM((5, fields, 320), F32),
            pltpu.SemaphoreType.DMA((7,)),
        ],
        name="inverse",
    )(late_half, level_wire, table)
    grids = [jnp.transpose(g, (1, 0, 2)) for g in grids]
    spectrum = jnp.transpose(spectrum.reshape(10, 2, fields, 641), (2, 1, 0, 3))
    return (spectrum, *grids)


def solution(mesh):
    return jax.shard_map(
        on_device,
        mesh=mesh,
        in_specs=(
            P("fld", "lat", None),
            P(),
            P(),
            P("lat", None, "fld"),
            P("lat", None, None),
            P("lat", None, None),
            P("lat", None, None),
        ),
        out_specs=(
            P("fld", None, "lat", None),
            P("fld", "lat", None),
            P("fld", "lat", None),
            P("fld", "lat", None),
        ),
        check_vma=False,
    )
```

```python
import math

import jax
import jax.numpy as jnp
from jax import lax
from jax.experimental import pallas as pl
from jax.experimental.pallas import tpu as pltpu
from jax.sharding import PartitionSpec as P


F32 = jnp.float32
BF16 = jnp.bfloat16

COS_TERMS = (
    1.0,
    -4.93480110168457,
    4.058694839477539,
    -1.3351584672927856,
    0.23502981662750244,
    -0.025358986109495163,
    0.0015939108561724424,
)
SIN_TERMS = (
    3.141592502593994,
    -5.167698860168457,
    2.5499982833862305,
    -0.5985506176948547,
    0.0807478278875351,
    -0.006089475005865097,
)

NT = (((1,), (1,)), ((), ()))
NN = (((1,), (0,)), ((), ()))


def turn(count, period):
    left = count - period * jnp.floor(count * (1.0 / period) + 0.5)
    place = left * (2.0 / period)
    square = place * place
    cosine = jnp.full_like(square, COS_TERMS[-1])
    for term in COS_TERMS[-2::-1]:
        cosine = cosine * square + term
    sine = jnp.full_like(square, SIN_TERMS[-1])
    for term in SIN_TERMS[-2::-1]:
        sine = sine * square + term
    return cosine, sine * place


def fill_table(wave, shift, scale, high_cos, high_sin, table_ref, period):
    count, width = table_ref.shape
    step = 16
    many = count // step
    low = lax.broadcasted_iota(jnp.int32, (step, width), 0).astype(F32)
    low_cos, low_sin = turn(low * wave, period)
    high = lax.broadcasted_iota(jnp.int32, (many, width), 0).astype(F32)
    first, second = turn(high * (wave * float(step)) + shift, period)
    high_cos[:many, :] = first * scale
    high_sin[:many, :] = second * scale

    def body(k, carry):
        value = high_cos[pl.ds(k, 1), :] * low_cos - high_sin[pl.ds(k, 1), :] * low_sin
        table_ref[pl.ds(pl.multiple_of(k * step, step), step), :] = value.astype(BF16)
        return carry

    lax.fori_loop(0, many, body, 0, unroll=4)


def identity(size):
    across = lax.broadcasted_iota(jnp.int32, (size, size), 0)
    along = lax.broadcasted_iota(jnp.int32, (size, size), 1)
    return jnp.where(across == along, 1.0, 0.0).astype(BF16)


def dft_kernel(
    info_ref,
    waves_ref,
    grid_hbm,
    wire_hbm,
    grid_ref,
    out_ref,
    even_ref,
    odd_ref,
    add_ref,
    sub_ref,
    turned_ref,
    high_cos,
    high_sin,
    in_sem,
    out_sem,
):
    half = grid_hbm.shape[1] // 2
    rows = grid_hbm.shape[0]
    incoming = pltpu.make_async_copy(grid_hbm, grid_ref, in_sem)
    incoming.start()
    lane = lax.broadcasted_iota(jnp.int32, (1, 768), 1).astype(F32)
    lane = lane - 24.0 * jnp.floor((lane + 0.5) * (1.0 / 24.0))
    size = 1.0 / math.sqrt(2 * half)
    for at, table_ref, first in ((0, even_ref, 0.0), (1, odd_ref, 4.0)):
        valid = (lane >= first) & (lane < first + 20.0)
        fill_table(
            waves_ref[at : at + 1, :],
            jnp.where(lane >= first + 10.0, half / 2.0, 0.0),
            jnp.where(valid, size, 0.0),
            high_cos,
            high_sin,
            table_ref,
            2 * half,
        )
    incoming.wait()

    def fold(k, carry):
        part = pl.ds(pl.multiple_of(k * 64, 64), 64)
        first = grid_ref[part, :half].astype(F32)
        second = grid_ref[part, half:].astype(F32)
        add_ref[part, :] = (first + second).astype(BF16)
        sub_ref[part, :] = (first - second).astype(BF16)
        return carry

    lax.fori_loop(0, rows // 64, fold, 0)
    add_ref[rows:, :] = jnp.zeros((1024 - rows, half), BF16)
    sub_ref[rows:, :] = jnp.zeros((1024 - rows, half), BF16)
    same = identity(128)
    turn_by = info_ref[0]
    shift = lax.rem(turn_by, 128)
    tile_shift = lax.div(turn_by, 128)
    lane = lax.broadcasted_iota(jnp.int32, (40, 128), 1)
    leaving = []
    for k in range(2):
        results = []
        for table_ref, folded_ref in ((even_ref, add_ref), (odd_ref, sub_ref)):
            for t in range(3):
                columns = slice(k * 384 + 128 * t, k * 384 + 128 * t + 128)
                turned_ref[128 * t : 128 * t + 128, :] = lax.dot_general(
                    same, table_ref[:, columns], NT, preferred_element_type=F32
                ).astype(BF16)
            results.append(
                lax.dot_general(turned_ref[...], folded_ref[...], NT, preferred_element_type=F32)
            )
        even, odd = results
        for d in range(16):
            one = even[24 * d : 24 * d + 24]
            two = odd[24 * d : 24 * d + 24]
            value = jnp.concatenate([one[:16], one[16:] + two[:8], two[8:]], axis=0)
            tiles = [pltpu.roll(value[:, 128 * t : 128 * t + 128], shift, 1) for t in range(8)]
            for t in range(8):
                tile = jnp.where(lane < shift, tiles[t - 1], tiles[t])
                place = pl.multiple_of(lax.rem(tile_shift + t, 8) * 128, 128)
                out_ref[k * 16 + d, :, pl.ds(place, 128)] = tile.astype(BF16)
        part = pl.ds(16 * k, 16)
        leaving.append(pltpu.make_async_copy(out_ref.at[part], wire_hbm.at[part], out_sem.at[k]))
        leaving[-1].start()
    for copy in leaving:
        copy.wait()


def pack_kernel(block_hbm, low_hbm, high_hbm, low_ref, high_ref, in_sem, out_sem):
    incoming = []
    for q in range(10):
        target = low_ref if q < 5 else high_ref
        incoming.append(
            pltpu.make_async_copy(
                block_hbm.at[q, :, pl.ds(0, 512)],
                target.at[pl.ds(q % 5 * 160, 160), :],
                in_sem.at[q],
            )
        )
        incoming[-1].start()
    for copy in incoming[:5]:
        copy.wait()
    low_out = pltpu.make_async_copy(low_ref, low_hbm, out_sem.at[0])
    low_out.start()
    for copy in incoming[5:]:
        copy.wait()
    high_out = pltpu.make_async_copy(high_ref, high_hbm, out_sem.at[1])
    high_out.start()
    low_out.wait()
    high_out.wait()


def pack_rest_kernel(block_hbm, rest_hbm, rest_ref, edge_ref, in_sem, out_sem):
    edge = pltpu.make_async_copy(block_hbm.at[:, :, pl.ds(640, 1)], edge_ref, in_sem.at[10])
    edge.start()
    incoming = []
    for q in range(10):
        incoming.append(
            pltpu.make_async_copy(
                block_hbm.at[q, :, pl.ds(512, 128)],
                rest_ref.at[pl.ds(q * 160, 160), :],
                in_sem.at[q],
            )
        )
        incoming[-1].start()
    edge.wait()
    lane = lax.broadcasted_iota(jnp.int32, (160, 128), 1)
    last = jnp.zeros((160, 128), F32)
    for q in range(10):
        last = jnp.where(lane == q, edge_ref[q].astype(F32), last)
    rest_ref[1600:, :] = last.astype(BF16)
    for copy in incoming:
        copy.wait()
    leaving = pltpu.make_async_copy(rest_ref, rest_hbm, out_sem)
    leaving.start()
    leaving.wait()


def lanes_kernel(wire_ref, out_ref, north_ref, south_ref):
    fields = north_ref.shape[1] // 40
    lane = lax.broadcasted_iota(jnp.int32, (40, 128), 1)
    for f in range(fields):
        offset = 40 * f % 128
        for half, target in ((0, north_ref), (16, south_ref)):
            tiles = []
            for o in range(6 if offset else 5):
                at = (40 * f // 128 + o) % 8 * 128
                first = 128 * o - offset
                tile = None
                for k in range(max(first // 40, 0), min((first + 127) // 40, 15) + 1):
                    piece = wire_ref[half + k, :, at : at + 128]
                    tile = piece if tile is None else jnp.where(lane >= 40 * k - first, piece, tile)
                tiles.append(tile.astype(F32))
            if offset:
                tiles = [pltpu.roll(tile, 128 - offset, 1) for tile in tiles]
                tiles = [
                    jnp.where(lane < 128 - offset, tiles[t], tiles[t + 1]) for t in range(5)
                ]
            for t in range(5):
                target[t, 40 * f : 40 * f + 40, :] = tiles[t]

    across = lax.broadcasted_iota(jnp.int32, (128, 128), 0)
    along = lax.broadcasted_iota(jnp.int32, (128, 128), 1)
    mirror = jnp.where(across + along == 127, 1.0, 0.0).astype(BF16)

    def fold(k, carry):
        rows = pl.ds(pl.multiple_of(k * 96, 96), 96)
        south = [
            lax.dot_general(
                south_ref[4 - t, rows, :].astype(BF16), mirror, NN, preferred_element_type=F32
            )
            for t in range(5)
        ]
        for t in range(5):
            first = north_ref[t, rows, :]
            north_ref[t, rows, :] = first + south[t]
            south_ref[t, rows, :] = first - south[t]
        return carry

    lax.fori_loop(0, north_ref.shape[1] // 96, fold, 0)

    def slot(q, carry):
        for t in range(5):
            parts = [
                source[t, pl.ds(g * 10 + q, fields, stride=40), :]
                for source in (north_ref, south_ref)
                for g in range(4)
            ]
            out_ref[q, :, 128 * t : 128 * t + 128] = jnp.concatenate(parts, axis=0).astype(BF16)
        return carry

    lax.fori_loop(0, out_ref.shape[0], slot, 0)


def turn_tables_kernel(one_ref, two_ref, three_ref, out_one, out_two, out_three, *picks):
    levels = ((one_ref, out_one, 4), (two_ref, out_two, 2), (three_ref, out_three, 1))

    @pl.when(pl.program_id(0) == 0)
    def _():
        for pick_ref, (source, _, groups) in zip(picks, levels):
            size = source.shape[1]
            row = lax.broadcasted_iota(jnp.int32, (size, size), 0)
            column = lax.broadcasted_iota(jnp.int32, (size, size), 1)
            b = row // (16 * groups)
            a = (row // 16) % groups
            place = (row % 16) * (5 * groups) + 5 * a + b
            pick_ref[...] = jnp.where(place == column, 1.0, 0.0).astype(BF16)

    for pick_ref, (source, target, _) in zip(picks, levels):
        target[0] = lax.dot_general(
            pick_ref[...], source[0], NT, preferred_element_type=F32
        ).astype(BF16)


def row_mask(condition, rows):
    value = jnp.where(condition, 1, 0)
    return jnp.broadcast_to(value, (rows, value.shape[1])) == 1


def slot_kernel(
    info_ref,
    waves_ref,
    own_low,
    left_low,
    right_low,
    far_low,
    own_high,
    left_high,
    right_high,
    far_high,
    one_ref,
    two_ref,
    three_ref,
    spectrum_hbm,
    wire_hbm,
    spectrum_ref,
    block_ref,
    pack_ref,
    wire_ref,
    spectrum_sem,
    block_sem,
    wire_sem,
):
    step = pl.program_id(0)
    x = info_ref[0]
    lows = (own_low, right_low, far_low, left_low)
    highs = (own_high, right_high, far_high, left_high)

    def copies(sources, q, first):
        out = []
        for k, source in enumerate(sources):
            place = pl.multiple_of(((x + k) % 4) * 160, 160)
            out.append(
                pltpu.make_async_copy(
                    source.at[pl.ds(pl.multiple_of((q - first) * 160, 160), 160), :],
                    block_ref.at[q % 4, pl.ds(place, 160), :],
                    block_sem.at[q % 4, k],
                )
            )
        return out

    def fetch(q):
        @pl.when(q < 5)
        def _():
            for copy in copies(lows, q, 0):
                copy.start()

        @pl.when(q >= 5)
        def _():
            for copy in copies(highs, q, 5):
                copy.start()

    @pl.when(step == 0)
    def _():
        fetch(2 * step)
        fetch(2 * step + 1)
        for row in range(140, 144):
            pack_ref[pl.ds(row, 32, stride=144), :] = jnp.zeros((32, 128), F32)

    @pl.when(step < 4)
    def _():
        fetch(2 * step + 2)
        fetch(2 * step + 3)

    slots = [2 * step, 2 * step + 1]
    orders = [info_ref[1 + q] for q in slots]
    for q in slots:
        for copy in copies(lows, q, q):
            copy.wait()

    rank = lax.broadcasted_iota(jnp.int32, (1, 512), 1)
    sym = rank < 321
    place = jnp.where(sym, rank, rank - 321)
    all_rows = []
    for k, (q, p) in enumerate(zip(slots, orders)):
        low = lax.dot_general(
            waves_ref[k, :96, :], block_ref[q % 4, :, :256], NN, preferred_element_type=F32
        )
        high = lax.dot_general(
            waves_ref[k], block_ref[q % 4, :, 256:], NN, preferred_element_type=F32
        )
        bound = jnp.where(sym, (641 - p) // 2, (640 - p) // 2)
        first = row_mask((place < bound) == (p % 2 == 0), 48)
        is_sym = row_mask(sym[:, 256:], 48)
        low = jnp.where(first[:, :256], low[:48], low[48:])
        high = jnp.where(
            is_sym,
            jnp.where(first[:, 256:], high[0:48], high[48:96]),
            jnp.where(first[:, 256:], high[96:144], high[144:192]),
        )
        chosen = jnp.concatenate([low, high], axis=1).astype(BF16)
        spectrum_ref[q] = chosen
        all_rows.append(chosen.astype(F32))
    group = 0
    for level, table_ref, count in ((0, one_ref, 4), (1, two_ref, 2), (2, three_ref, 1)):
        size = table_ref.shape[1]
        half = size // 2
        limit = info_ref[11 + level]
        lane = lax.broadcasted_iota(jnp.int32, (1, size), 1)
        is_sym = lane < half
        sym_rows = row_mask(is_sym, 48)
        extra = jnp.where(is_sym, 2 * lane, 2 * (lane - half) + 1)
        many = 16 * count
        wide = lax.broadcasted_iota(jnp.int32, (many, 128), 1)
        for k, (q, p) in enumerate(zip(slots, orders)):
            rows = all_rows[k]
            later = pltpu.roll(rows, 512 - 321 + half, 1)[:, :size]
            keep = row_mask(p + extra <= limit, 48)
            kept = jnp.where(keep, jnp.where(sym_rows, rows[:, :size], later), 0.0)
            both = jnp.concatenate(
                [kept, jnp.where(sym_rows, kept, -kept), jnp.zeros((32, size), F32)], axis=0
            ).astype(BF16)
            value = lax.dot_general(table_ref[k], both, NT, preferred_element_type=F32)
            for sign in range(2):
                for c in range(2):
                    packed = None
                    for b in range(5):
                        part = value[many * b : many * b + many]
                        move = 24 * (b - 2 * sign - c) % 128
                        if move:
                            part = pltpu.roll(part, move, 1)
                        packed = part if b == 0 else jnp.where(wide >= 24 * b, part, packed)
                    for a in range(count):
                        start = sign * 16 * 144 + 20 * (group + a) + 10 * c + q
                        pack_ref[pl.ds(start, 16, stride=144), :] = packed[16 * a : 16 * a + 16]
        group += count

    @pl.when(step == pl.num_programs(0) - 1)
    def _():
        for d in range(16):
            wire_ref[d] = pack_ref[144 * d : 144 * d + 144, :].astype(BF16)
            wire_ref[31 - d] = pack_ref[144 * (16 + d) : 144 * (17 + d), :].astype(BF16)
        leaving = [
            pltpu.make_async_copy(wire_ref, wire_hbm, wire_sem),
            pltpu.make_async_copy(spectrum_ref, spectrum_hbm, spectrum_sem),
        ]
        for copy in leaving:
            copy.start()
        for copy in leaving:
            copy.wait()


def rest_kernel(
    info_ref, waves_ref, own_ref, left_ref, right_ref, far_ref, out_ref, block_ref, edge_ref
):
    x = info_ref[0]
    for k, source in enumerate((own_ref, right_ref, far_ref, left_ref)):
        place = pl.multiple_of(((x + k) % 4) * 160, 160)
        for q in range(10):
            block_ref[q, pl.ds(place, 160), :] = source[160 * q : 160 * q + 160, :]
        edge_ref[pl.ds(place, 160), :] = source[1600:, :]
    rank = lax.broadcasted_iota(jnp.int32, (1, 128), 1) + (512 - 321)
    lane = lax.broadcasted_iota(jnp.int32, (48, 128), 1)

    def slot(q, carry):
        p = info_ref[1 + q]
        left = waves_ref[q, 96:, :]
        even_pair = p % 2 == 0
        bound = (640 - p) // 2
        value = lax.dot_general(left, block_ref[q], NN, preferred_element_type=F32)
        first = row_mask((rank < bound) == even_pair, 48)
        out_ref[q, :, :128] = jnp.where(first, value[:48], value[48:]).astype(BF16)
        value = lax.dot_general(left, edge_ref[...], NN, preferred_element_type=F32)
        value = jnp.where(((319 < bound) == even_pair) & (lane >= 0), value[:48], value[48:])
        out_ref[q, :, 128:] = pltpu.roll(value, lax.rem(128 - q, 128), 1)[:, :1].astype(BF16)
        return carry

    lax.fori_loop(0, 10, slot, 0)


def inverse_table_kernel(waves_ref, table_ref, high_cos, high_sin):
    wave = waves_ref[0:1, :]
    lane = lax.broadcasted_iota(jnp.int32, (1, 768), 1).astype(F32)
    lane = lane - 24.0 * jnp.floor((lane + 0.5) * (1.0 / 24.0))
    weight = jnp.where(lane < 20.0, jnp.where(wave == 0.0, 1.0, 2.0), 0.0)
    first = 0
    for period in (1280, 640, 320):
        shift = jnp.where(lane >= 10.0, period / 4.0, 0.0)
        scale = weight * (1.0 / math.sqrt(period))
        part = table_ref.at[pl.ds(first, period), :]
        fill_table(wave, shift, scale, high_cos, high_sin, part, period)
        first += period


def inverse_kernel(
    info_ref,
    wire_ref,
    table_ref,
    out_one,
    out_two,
    out_three,
    big_ref,
    mid_ref,
    small_ref,
    out_sem,
):
    late_half = info_ref[0]
    same = identity(128)

    def lines(group):
        start = 20 * group // 8 * 8
        part = wire_ref[:, start : start + 24, :].astype(F32)
        if 20 * group > start:
            part = pltpu.roll(part, 24 - (20 * group - start), 1)
        part = part.reshape(part.shape[0] * 24, 128).astype(BF16)
        return lax.dot_general(same, part, NT, preferred_element_type=F32).astype(BF16)

    def place(target, value, count, last):
        for a in range(count):
            for b in range(5):
                row = 5 * a + b
                row = jnp.where(late_half == 1, last - row, row)
                target[row] = value[128 * a + 24 * b : 128 * a + 24 * b + 24]

    leaving = []

    def leave(source, target):
        copy = pltpu.make_async_copy(source, target, out_sem.at[len(leaving)])
        copy.start()
        leaving.append(copy)

    left = [lines(group) for group in range(7)]
    value = lax.dot_general(left[6], table_ref[1920:, :], NT, preferred_element_type=F32)
    place(small_ref, value, 1, 4)
    leave(small_ref, out_three)
    value = lax.dot_general(
        jnp.concatenate(left[4:6], axis=0),
        table_ref[1280:1920, :],
        NT,
        preferred_element_type=F32,
    )
    place(mid_ref, value, 2, 9)
    leave(mid_ref, out_two)
    left = jnp.concatenate(left[:4], axis=0)
    for n in range(5):
        columns = slice(256 * n, 256 * n + 256)
        value = lax.dot_general(left, table_ref[columns, :], NT, preferred_element_type=F32)
        place(big_ref.at[n], value, 4, 19)
        leave(big_ref.at[n], out_one.at[:, :, pl.ds(256 * n, 256)])
    for copy in leaving:
        copy.wait()


def call(kernel, out_shape, limit, **kw):
    return pl.pallas_call(
        kernel,
        out_shape=out_shape,
        compiler_params=pltpu.CompilerParams(vmem_limit_bytes=limit * 1024 * 1024),
        **kw,
    )


def on_device(grid_fields, assign, limits, legendre, synth_one, synth_two, synth_three):
    fields, rows, lon = grid_fields.shape
    lat_at = lax.axis_index("lat")
    fld_at = lax.axis_index("fld")
    vmem = pl.BlockSpec(memory_space=pltpu.VMEM)

    hbm = pl.BlockSpec(memory_space=pltpu.HBM)
    own = jnp.transpose(legendre, (0, 2, 1))
    low, high = call(
        pack_kernel,
        [jax.ShapeDtypeStruct((800, 512), BF16)] * 2,
        60,
        in_specs=[hbm],
        out_specs=[hbm, hbm],
        scratch_shapes=[
            pltpu.VMEM((800, 512), BF16),
            pltpu.VMEM((800, 512), BF16),
            pltpu.SemaphoreType.DMA((10,)),
            pltpu.SemaphoreType.DMA((2,)),
        ],
        name="pack",
    )(own)
    low, high, grid_fields, assign = lax.optimization_barrier((low, high, grid_fields, assign))
    right = [(k, (k + 1) % 4) for k in range(4)]
    left = [(k, (k + 3) % 4) for k in range(4)]
    across = [(k, (k + 2) % 4) for k in range(4)]
    low_left = lax.ppermute(low, "fld", right)
    high_right = lax.ppermute(high, "fld", left)
    low_right = lax.ppermute(low, "fld", left)
    high_left = lax.ppermute(high, "fld", right)
    low_far = lax.ppermute(low_left, "fld", right)
    high_far = lax.ppermute(high_right, "fld", left)

    pairs = assign.reshape(32, 10)
    even = jnp.where(pairs % 2 == 0, pairs, 639 - pairs).astype(F32)
    odd = 639.0 - even
    spare = jnp.zeros((32, 4), F32)
    forward_waves = jnp.stack(
        [
            jnp.concatenate([even, even, spare], axis=1),
            jnp.concatenate([spare, odd, odd], axis=1),
        ]
    ).reshape(2, 768)
    wire = call(
        dft_kernel,
        jax.ShapeDtypeStruct((32, 40, 1024), BF16),
        60,
        in_specs=[pl.BlockSpec(memory_space=pltpu.SMEM), vmem, hbm],
        out_specs=hbm,
        scratch_shapes=[
            pltpu.VMEM((fields * rows, lon), BF16),
            pltpu.VMEM((32, 40, 1024), BF16),
            pltpu.VMEM((lon // 2, 768), BF16),
            pltpu.VMEM((lon // 2, 768), BF16),
            pltpu.VMEM((1024, lon // 2), BF16),
            pltpu.VMEM((1024, lon // 2), BF16),
            pltpu.VMEM((384, lon // 2), BF16),
            pltpu.VMEM((80, 768), F32),
            pltpu.VMEM((80, 768), F32),
            pltpu.SemaphoreType.DMA(()),
            pltpu.SemaphoreType.DMA((2,)),
        ],
        name="dft",
    )((lat_at % 16 * 40).reshape(1), forward_waves, grid_fields.reshape(fields * rows, lon))
    assign_after, synth_one, synth_two, synth_three, own, wire = lax.optimization_barrier(
        (assign, synth_one, synth_two, synth_three, own, wire)
    )
    wire = lax.all_to_all(wire, "lat", split_axis=0, concat_axis=0, tiled=True)

    rest = call(
        pack_rest_kernel,
        jax.ShapeDtypeStruct((1760, 128), BF16),
        60,
        in_specs=[hbm],
        out_specs=hbm,
        scratch_shapes=[
            pltpu.VMEM((1760, 128), BF16),
            pltpu.VMEM((10, 160, 1), BF16),
            pltpu.SemaphoreType.DMA((11,)),
            pltpu.SemaphoreType.DMA(()),
        ],
        name="pack_rest",
    )(own)
    rest_left = lax.ppermute(rest, "fld", right)
    rest_right = lax.ppermute(rest, "fld", left)
    rest_far = lax.ppermute(rest, "fld", across)

    synths = (synth_one, synth_two, synth_three)
    slot_block = [pl.BlockSpec((1,) + t.shape[1:], lambda q: (q, 0, 0)) for t in synths]
    turned = call(
        turn_tables_kernel,
        [jax.ShapeDtypeStruct(t.shape, BF16) for t in synths],
        60,
        grid=(10,),
        in_specs=slot_block,
        out_specs=slot_block,
        scratch_shapes=[pltpu.VMEM(t.shape[1:], BF16) for t in synths],
        name="turn_tables",
    )(*synths)

    waves = call(
        lanes_kernel,
        jax.ShapeDtypeStruct((10, 192, 640), BF16),
        18,
        in_specs=[vmem],
        out_specs=vmem,
        scratch_shapes=[
            pltpu.VMEM((5, fields * rows, 128), F32),
            pltpu.VMEM((5, fields * rows, 128), F32),
        ],
        name="lanes",
    )(wire)

    info = jnp.concatenate(
        [fld_at.reshape(1), lax.dynamic_slice_in_dim(assign_after, lat_at * 10, 10), limits]
    )
    spectrum, level_wire = call(
        slot_kernel,
        [
            jax.ShapeDtypeStruct((10, 2 * fields, 512), BF16),
            jax.ShapeDtypeStruct((32, 144, 128), BF16),
        ],
        60,
        grid_spec=pltpu.PrefetchScalarGridSpec(
            num_scalar_prefetch=1,
            grid=(5,),
            in_specs=[pl.BlockSpec((2, 192, 640), lambda q, *_: (q, 0, 0))]
            + [hbm] * 8
            + [pl.BlockSpec((2,) + t.shape[1:], lambda q, *_: (q, 0, 0)) for t in turned],
            out_specs=[hbm, hbm],
            scratch_shapes=[
                pltpu.VMEM((10, 2 * fields, 512), BF16),
                pltpu.VMEM((4, 640, 512), BF16),
                pltpu.VMEM((32 * 144, 128), F32),
                pltpu.VMEM((32, 144, 128), BF16),
                pltpu.SemaphoreType.DMA(()),
                pltpu.SemaphoreType.DMA((4, 4)),
                pltpu.SemaphoreType.DMA(()),
            ],
        ),
        name="slots",
    )(
        info,
        waves,
        low,
        low_left,
        low_right,
        low_far,
        high,
        high_left,
        high_right,
        high_far,
        *turned,
    )
    info, waves, level_wire = lax.optimization_barrier((info, waves, level_wire))
    rest_spectrum = call(
        rest_kernel,
        jax.ShapeDtypeStruct((10, 2 * fields, 129), BF16),
        16,
        in_specs=[pl.BlockSpec(memory_space=pltpu.SMEM)] + [vmem] * 5,
        out_specs=vmem,
        scratch_shapes=[pltpu.VMEM((10, 640, 128), BF16), pltpu.VMEM((640, 128), BF16)],
        name="rest",
    )(info, waves, rest, rest_left, rest_right, rest_far)
    level_wire = lax.all_to_all(level_wire, "lat", split_axis=0, concat_axis=0, tiled=True)
    assign_late, rest_spectrum = lax.optimization_barrier((assign, rest_spectrum))
    plain = assign_late.reshape(32, 10).astype(F32)
    spare = jnp.zeros((32, 4), F32)
    inverse_waves = jnp.concatenate([plain, plain, spare], axis=1).reshape(1, 768)
    table = call(
        inverse_table_kernel,
        jax.ShapeDtypeStruct((2240, 768), BF16),
        12,
        in_specs=[vmem],
        out_specs=vmem,
        scratch_shapes=[pltpu.VMEM((80, 768), F32), pltpu.VMEM((80, 768), F32)],
        name="inverse_tables",
    )(inverse_waves)


    late_half = (lat_at >= 16).astype(jnp.int32).reshape(1)
    grids = call(
        inverse_kernel,
        [
            jax.ShapeDtypeStruct((20, fields, 1280), F32),
            jax.ShapeDtypeStruct((10, fields, 640), F32),
            jax.ShapeDtypeStruct((5, fields, 320), F32),
        ],
        24,
        in_specs=[pl.BlockSpec(memory_space=pltpu.SMEM), vmem, vmem],
        out_specs=[hbm] * 3,
        scratch_shapes=[
            pltpu.VMEM((5, 20, fields, 256), F32),
            pltpu.VMEM((10, fields, 640), F32),
            pltpu.VMEM((5, fields, 320), F32),
            pltpu.SemaphoreType.DMA((7,)),
        ],
        name="inverse",
    )(late_half, level_wire, table)
    grids = [jnp.transpose(g, (1, 0, 2)) for g in grids]
    spectrum = jnp.concatenate([spectrum, rest_spectrum], axis=2).reshape(10, 2, fields, 641)
    spectrum = jnp.transpose(spectrum, (2, 1, 0, 3))
    return (spectrum, *grids)


def solution(mesh):
    return jax.shard_map(
        on_device,
        mesh=mesh,
        in_specs=(
            P("fld", "lat", None),
            P(),
            P(),
            P("lat", None, "fld"),
            P("lat", None, None),
            P("lat", None, None),
            P("lat", None, None),
        ),
        out_specs=(
            P("fld", None, "lat", None),
            P("fld", "lat", None),
            P("fld", "lat", None),
            P("fld", "lat", None),
        ),
        check_vma=False,
    )
```

```python
import math

import jax
import jax.numpy as jnp
from jax import lax
from jax.experimental import pallas as pl
from jax.experimental.pallas import tpu as pltpu
from jax.sharding import PartitionSpec as P


F32 = jnp.float32
BF16 = jnp.bfloat16

COS_TERMS = (
    1.0,
    -4.93480110168457,
    4.058694839477539,
    -1.3351584672927856,
    0.23502981662750244,
    -0.025358986109495163,
    0.0015939108561724424,
)
SIN_TERMS = (
    3.141592502593994,
    -5.167698860168457,
    2.5499982833862305,
    -0.5985506176948547,
    0.0807478278875351,
    -0.006089475005865097,
)

NT = (((1,), (1,)), ((), ()))
NN = (((1,), (0,)), ((), ()))


def turn(count, period):
    left = count - period * jnp.floor(count * (1.0 / period) + 0.5)
    place = left * (2.0 / period)
    square = place * place
    cosine = jnp.full_like(square, COS_TERMS[-1])
    for term in COS_TERMS[-2::-1]:
        cosine = cosine * square + term
    sine = jnp.full_like(square, SIN_TERMS[-1])
    for term in SIN_TERMS[-2::-1]:
        sine = sine * square + term
    return cosine, sine * place


def fill_table(wave, shift, scale, high_cos, high_sin, table_ref, period):
    count, width = table_ref.shape
    step = 16
    many = count // step
    low = lax.broadcasted_iota(jnp.int32, (step, width), 0).astype(F32)
    low_cos, low_sin = turn(low * wave, period)
    high = lax.broadcasted_iota(jnp.int32, (many, width), 0).astype(F32)
    first, second = turn(high * (wave * float(step)) + shift, period)
    high_cos[:many, :] = first * scale
    high_sin[:many, :] = second * scale

    def body(k, carry):
        value = high_cos[pl.ds(k, 1), :] * low_cos - high_sin[pl.ds(k, 1), :] * low_sin
        table_ref[pl.ds(pl.multiple_of(k * step, step), step), :] = value.astype(BF16)
        return carry

    lax.fori_loop(0, many, body, 0, unroll=4)


def identity(size):
    across = lax.broadcasted_iota(jnp.int32, (size, size), 0)
    along = lax.broadcasted_iota(jnp.int32, (size, size), 1)
    return jnp.where(across == along, 1.0, 0.0).astype(BF16)


def dft_kernel(
    info_ref,
    waves_ref,
    grid_hbm,
    wire_hbm,
    grid_ref,
    out_ref,
    even_ref,
    odd_ref,
    add_ref,
    sub_ref,
    turned_ref,
    high_cos,
    high_sin,
    in_sem,
    out_sem,
):
    half = grid_hbm.shape[1] // 2
    rows = grid_hbm.shape[0]
    incoming = pltpu.make_async_copy(grid_hbm, grid_ref, in_sem)
    incoming.start()
    lane = lax.broadcasted_iota(jnp.int32, (1, 768), 1).astype(F32)
    lane = lane - 24.0 * jnp.floor((lane + 0.5) * (1.0 / 24.0))
    size = 1.0 / math.sqrt(2 * half)
    for at, table_ref, first in ((0, even_ref, 0.0), (1, odd_ref, 4.0)):
        valid = (lane >= first) & (lane < first + 20.0)
        fill_table(
            waves_ref[at : at + 1, :],
            jnp.where(lane >= first + 10.0, half / 2.0, 0.0),
            jnp.where(valid, size, 0.0),
            high_cos,
            high_sin,
            table_ref,
            2 * half,
        )
    incoming.wait()

    def fold(k, carry):
        part = pl.ds(pl.multiple_of(k * 64, 64), 64)
        first = grid_ref[part, :half].astype(F32)
        second = grid_ref[part, half:].astype(F32)
        add_ref[part, :] = (first + second).astype(BF16)
        sub_ref[part, :] = (first - second).astype(BF16)
        return carry

    lax.fori_loop(0, rows // 64, fold, 0)
    add_ref[rows:, :] = jnp.zeros((1024 - rows, half), BF16)
    sub_ref[rows:, :] = jnp.zeros((1024 - rows, half), BF16)
    same = identity(128)
    turn_by = info_ref[0]
    shift = lax.rem(turn_by, 128)
    tile_shift = lax.div(turn_by, 128)
    lane = lax.broadcasted_iota(jnp.int32, (40, 128), 1)
    leaving = []
    for k in range(2):
        results = []
        for table_ref, folded_ref in ((even_ref, add_ref), (odd_ref, sub_ref)):
            for t in range(3):
                columns = slice(k * 384 + 128 * t, k * 384 + 128 * t + 128)
                turned_ref[128 * t : 128 * t + 128, :] = lax.dot_general(
                    same, table_ref[:, columns], NT, preferred_element_type=F32
                ).astype(BF16)
            results.append(
                lax.dot_general(turned_ref[...], folded_ref[...], NT, preferred_element_type=F32)
            )
        even, odd = results
        for d in range(16):
            one = even[24 * d : 24 * d + 24]
            two = odd[24 * d : 24 * d + 24]
            value = jnp.concatenate([one[:16], one[16:] + two[:8], two[8:]], axis=0)
            tiles = [pltpu.roll(value[:, 128 * t : 128 * t + 128], shift, 1) for t in range(8)]
            for t in range(8):
                tile = jnp.where(lane < shift, tiles[t - 1], tiles[t])
                place = pl.multiple_of(lax.rem(tile_shift + t, 8) * 128, 128)
                out_ref[k * 16 + d, :, pl.ds(place, 128)] = tile.astype(BF16)
        part = pl.ds(16 * k, 16)
        leaving.append(pltpu.make_async_copy(out_ref.at[part], wire_hbm.at[part], out_sem.at[k]))
        leaving[-1].start()
    for copy in leaving:
        copy.wait()


def pack_kernel(block_hbm, low_hbm, high_hbm, low_ref, high_ref, in_sem, out_sem):
    incoming = []
    for q in range(10):
        target = low_ref if q < 5 else high_ref
        incoming.append(
            pltpu.make_async_copy(
                block_hbm.at[q, :, pl.ds(0, 512)],
                target.at[pl.ds(q % 5 * 160, 160), :],
                in_sem.at[q],
            )
        )
        incoming[-1].start()
    for copy in incoming[:5]:
        copy.wait()
    low_out = pltpu.make_async_copy(low_ref, low_hbm, out_sem.at[0])
    low_out.start()
    for copy in incoming[5:]:
        copy.wait()
    high_out = pltpu.make_async_copy(high_ref, high_hbm, out_sem.at[1])
    high_out.start()
    low_out.wait()
    high_out.wait()


def pack_rest_kernel(block_hbm, rest_hbm, rest_ref, edge_ref, in_sem, out_sem):
    edge = pltpu.make_async_copy(block_hbm.at[:, :, pl.ds(640, 1)], edge_ref, in_sem.at[10])
    edge.start()
    incoming = []
    for q in range(10):
        incoming.append(
            pltpu.make_async_copy(
                block_hbm.at[q, :, pl.ds(512, 128)],
                rest_ref.at[pl.ds(q * 160, 160), :],
                in_sem.at[q],
            )
        )
        incoming[-1].start()
    edge.wait()
    lane = lax.broadcasted_iota(jnp.int32, (160, 128), 1)
    last = jnp.zeros((160, 128), F32)
    for q in range(10):
        last = jnp.where(lane == q, edge_ref[q].astype(F32), last)
    rest_ref[1600:, :] = last.astype(BF16)
    for copy in incoming:
        copy.wait()
    leaving = pltpu.make_async_copy(rest_ref, rest_hbm, out_sem)
    leaving.start()
    leaving.wait()


def turn_tables_kernel(one_ref, two_ref, three_ref, out_one, out_two, out_three, *picks):
    levels = ((one_ref, out_one, 4), (two_ref, out_two, 2), (three_ref, out_three, 1))

    @pl.when(pl.program_id(0) == 0)
    def _():
        for pick_ref, (source, _, groups) in zip(picks, levels):
            size = source.shape[1]
            row = lax.broadcasted_iota(jnp.int32, (size, size), 0)
            column = lax.broadcasted_iota(jnp.int32, (size, size), 1)
            b = row // (16 * groups)
            a = (row // 16) % groups
            place = (row % 16) * (5 * groups) + 5 * a + b
            pick_ref[...] = jnp.where(place == column, 1.0, 0.0).astype(BF16)

    for pick_ref, (source, target, _) in zip(picks, levels):
        target[0] = lax.dot_general(
            pick_ref[...], source[0], NT, preferred_element_type=F32
        ).astype(BF16)


def row_mask(condition, rows):
    value = jnp.where(condition, 1, 0)
    return jnp.broadcast_to(value, (rows, value.shape[1])) == 1


def level_kernel(
    info_ref,
    arrived_hbm,
    own_low,
    left_low,
    right_low,
    far_low,
    own_high,
    left_high,
    right_high,
    far_high,
    one_hbm,
    two_hbm,
    three_hbm,
    spectrum_hbm,
    wire_hbm,
    waves_hbm,
    north_ref,
    south_ref,
    waves_ref,
    block_ref,
    one_ref,
    two_ref,
    three_ref,
    spectrum_ref,
    pack_ref,
    wire_ref,
    arrived_ref,
    arrived_sem,
    block_sem,
    table_sem,
    out_sem,
):
    x = info_ref[0]
    arriving = [
        pltpu.make_async_copy(
            arrived_hbm.at[pl.ds(16 * k, 16)], arrived_ref.at[pl.ds(16 * k, 16)], arrived_sem.at[k]
        )
        for k in range(2)
    ]
    for copy in arriving:
        copy.start()
    lows = (own_low, right_low, far_low, left_low)
    highs = (own_high, right_high, far_high, left_high)

    def block_copy(source, q, place, k):
        return pltpu.make_async_copy(
            source.at[pl.ds(q % 5 * 160, 160), :],
            block_ref.at[q, pl.ds(place, 160), :],
            block_sem.at[q, k],
        )

    tables = [
        pltpu.make_async_copy(source, target, table_sem.at[k])
        for k, (source, target) in enumerate(
            ((one_hbm, one_ref), (two_hbm, two_ref), (three_hbm, three_ref))
        )
    ]
    for q in range(10):
        for k, source in enumerate(lows if q < 5 else highs):
            block_copy(source, q, pl.multiple_of(((x + k) % 4) * 160, 160), k).start()
        if q == 1:
            for copy in tables:
                copy.start()
    for row in range(140, 144):
        pack_ref[pl.ds(row, 32, stride=144), :] = jnp.zeros((32, 128), F32)

    fields = north_ref.shape[1] // 40
    lane = lax.broadcasted_iota(jnp.int32, (40, 128), 1)
    for half, target in ((0, north_ref), (16, south_ref)):
        arriving[half // 16].wait()
        for f in range(fields):
            offset = 40 * f % 128
            tiles = []
            for o in range(6 if offset else 5):
                at = (40 * f // 128 + o) % 8 * 128
                first = 128 * o - offset
                tile = None
                for k in range(max(first // 40, 0), min((first + 127) // 40, 15) + 1):
                    piece = arrived_ref[half + k, :, at : at + 128]
                    tile = piece if tile is None else jnp.where(lane >= 40 * k - first, piece, tile)
                tiles.append(tile.astype(F32))
            if offset:
                tiles = [pltpu.roll(tile, 128 - offset, 1) for tile in tiles]
                tiles = [
                    jnp.where(lane < 128 - offset, tiles[t], tiles[t + 1]) for t in range(5)
                ]
            for t in range(5):
                target[t, 40 * f : 40 * f + 40, :] = tiles[t]

    across = lax.broadcasted_iota(jnp.int32, (128, 128), 0)
    along = lax.broadcasted_iota(jnp.int32, (128, 128), 1)
    mirror = jnp.where(across + along == 127, 1.0, 0.0).astype(BF16)

    def fold(k, carry):
        rows = pl.ds(pl.multiple_of(k * 96, 96), 96)
        south = [
            lax.dot_general(
                south_ref[4 - t, rows, :].astype(BF16), mirror, NN, preferred_element_type=F32
            )
            for t in range(5)
        ]
        for t in range(5):
            first = north_ref[t, rows, :]
            north_ref[t, rows, :] = first + south[t]
            south_ref[t, rows, :] = first - south[t]
        return carry

    lax.fori_loop(0, north_ref.shape[1] // 96, fold, 0)

    def slot(q, carry):
        for t in range(5):
            parts = [
                source[t, pl.ds(g * 10 + q, fields, stride=40), :]
                for source in (north_ref, south_ref)
                for g in range(4)
            ]
            waves_ref[q, :, 128 * t : 128 * t + 128] = jnp.concatenate(parts, axis=0).astype(BF16)
        return carry

    lax.fori_loop(0, 10, slot, 0)

    waves_out = pltpu.make_async_copy(waves_ref, waves_hbm, out_sem.at[0])
    waves_out.start()
    for copy in tables:
        copy.wait()
    rank = lax.broadcasted_iota(jnp.int32, (1, 512), 1)
    sym = rank < 321
    place = jnp.where(sym, rank, rank - 321)

    def two_slots(step, carry):
        slots = [2 * step, 2 * step + 1]
        orders = [info_ref[1 + q] for q in slots]
        for q in slots:
            for k, source in enumerate(lows):
                pltpu.make_async_copy(
                    source.at[pl.ds(0, 160), :], block_ref.at[q, pl.ds(0, 160), :], block_sem.at[q, k]
                ).wait()
        all_rows = []
        for q, p in zip(slots, orders):
            low = lax.dot_general(
                waves_ref[q, :96, :], block_ref[q, :, :256], NN, preferred_element_type=F32
            )
            high = lax.dot_general(
                waves_ref[q], block_ref[q, :, 256:], NN, preferred_element_type=F32
            )
            bound = jnp.where(sym, (641 - p) // 2, (640 - p) // 2)
            first = row_mask((place < bound) == (p % 2 == 0), 48)
            is_sym = row_mask(sym[:, 256:], 48)
            low = jnp.where(first[:, :256], low[:48], low[48:])
            high = jnp.where(
                is_sym,
                jnp.where(first[:, 256:], high[0:48], high[48:96]),
                jnp.where(first[:, 256:], high[96:144], high[144:192]),
            )
            chosen = jnp.concatenate([low, high], axis=1).astype(BF16)
            spectrum_ref[q] = chosen
            all_rows.append(chosen.astype(F32))
        group = 0
        for level, table_ref, count in ((0, one_ref, 4), (1, two_ref, 2), (2, three_ref, 1)):
            size = table_ref.shape[1]
            half = size // 2
            limit = info_ref[11 + level]
            lane = lax.broadcasted_iota(jnp.int32, (1, size), 1)
            is_sym = lane < half
            sym_rows = row_mask(is_sym, 48)
            extra = jnp.where(is_sym, 2 * lane, 2 * (lane - half) + 1)
            many = 16 * count
            wide = lax.broadcasted_iota(jnp.int32, (many, 128), 1)
            for k, (q, p) in enumerate(zip(slots, orders)):
                rows = all_rows[k]
                later = pltpu.roll(rows, 512 - 321 + half, 1)[:, :size]
                keep = row_mask(p + extra <= limit, 48)
                kept = jnp.where(keep, jnp.where(sym_rows, rows[:, :size], later), 0.0)
                both = jnp.concatenate(
                    [kept, jnp.where(sym_rows, kept, -kept), jnp.zeros((32, size), F32)], axis=0
                ).astype(BF16)
                value = lax.dot_general(table_ref[q], both, NT, preferred_element_type=F32)
                for sign in range(2):
                    for c in range(2):
                        packed = None
                        for b in range(5):
                            part = value[many * b : many * b + many]
                            move = 24 * (b - 2 * sign - c) % 128
                            if move:
                                part = pltpu.roll(part, move, 1)
                            packed = part if b == 0 else jnp.where(wide >= 24 * b, part, packed)
                        for a in range(count):
                            start = sign * 16 * 144 + 20 * (group + a) + 10 * c + q
                            pack_ref[pl.ds(start, 16, stride=144), :] = packed[16 * a : 16 * a + 16]
            group += count

        return carry

    lax.fori_loop(0, 5, two_slots, 0)
    for d in range(16):
        wire_ref[d] = pack_ref[144 * d : 144 * d + 144, :].astype(BF16)
        wire_ref[31 - d] = pack_ref[144 * (16 + d) : 144 * (17 + d), :].astype(BF16)
    leaving = [
        pltpu.make_async_copy(wire_ref, wire_hbm, out_sem.at[1]),
        pltpu.make_async_copy(spectrum_ref, spectrum_hbm, out_sem.at[2]),
    ]
    for copy in leaving:
        copy.start()
    for copy in leaving:
        copy.wait()
    waves_out.wait()


def rest_kernel(
    info_ref, waves_ref, own_ref, left_ref, right_ref, far_ref, out_ref, block_ref, edge_ref
):
    x = info_ref[0]
    for k, source in enumerate((own_ref, right_ref, far_ref, left_ref)):
        place = pl.multiple_of(((x + k) % 4) * 160, 160)
        for q in range(10):
            block_ref[q, pl.ds(place, 160), :] = source[160 * q : 160 * q + 160, :]
        edge_ref[pl.ds(place, 160), :] = source[1600:, :]
    rank = lax.broadcasted_iota(jnp.int32, (1, 128), 1) + (512 - 321)
    lane = lax.broadcasted_iota(jnp.int32, (48, 128), 1)

    def slot(q, carry):
        p = info_ref[1 + q]
        left = waves_ref[q, 96:, :]
        even_pair = p % 2 == 0
        bound = (640 - p) // 2
        value = lax.dot_general(left, block_ref[q], NN, preferred_element_type=F32)
        first = row_mask((rank < bound) == even_pair, 48)
        out_ref[q, :, :128] = jnp.where(first, value[:48], value[48:]).astype(BF16)
        value = lax.dot_general(left, edge_ref[...], NN, preferred_element_type=F32)
        value = jnp.where(((319 < bound) == even_pair) & (lane >= 0), value[:48], value[48:])
        out_ref[q, :, 128:] = pltpu.roll(value, lax.rem(128 - q, 128), 1)[:, :1].astype(BF16)
        return carry

    lax.fori_loop(0, 10, slot, 0)


def inverse_table_kernel(waves_ref, table_ref, high_cos, high_sin):
    wave = waves_ref[0:1, :]
    lane = lax.broadcasted_iota(jnp.int32, (1, 768), 1).astype(F32)
    lane = lane - 24.0 * jnp.floor((lane + 0.5) * (1.0 / 24.0))
    weight = jnp.where(lane < 20.0, jnp.where(wave == 0.0, 1.0, 2.0), 0.0)
    first = 0
    for period in (1280, 640, 320):
        shift = jnp.where(lane >= 10.0, period / 4.0, 0.0)
        scale = weight * (1.0 / math.sqrt(period))
        part = table_ref.at[pl.ds(first, period), :]
        fill_table(wave, shift, scale, high_cos, high_sin, part, period)
        first += period


def inverse_kernel(
    info_ref,
    wire_ref,
    table_ref,
    out_one,
    out_two,
    out_three,
    big_ref,
    mid_ref,
    small_ref,
    out_sem,
):
    late_half = info_ref[0]
    same = identity(128)

    def lines(group):
        start = 20 * group // 8 * 8
        part = wire_ref[:, start : start + 24, :].astype(F32)
        if 20 * group > start:
            part = pltpu.roll(part, 24 - (20 * group - start), 1)
        part = part.reshape(part.shape[0] * 24, 128).astype(BF16)
        return lax.dot_general(same, part, NT, preferred_element_type=F32).astype(BF16)

    def place(target, value, count, last):
        for a in range(count):
            for b in range(5):
                row = 5 * a + b
                row = jnp.where(late_half == 1, last - row, row)
                target[row] = value[128 * a + 24 * b : 128 * a + 24 * b + 24]

    leaving = []

    def leave(source, target):
        copy = pltpu.make_async_copy(source, target, out_sem.at[len(leaving)])
        copy.start()
        leaving.append(copy)

    left = [lines(group) for group in range(7)]
    value = lax.dot_general(left[6], table_ref[1920:, :], NT, preferred_element_type=F32)
    place(small_ref, value, 1, 4)
    leave(small_ref, out_three)
    value = lax.dot_general(
        jnp.concatenate(left[4:6], axis=0),
        table_ref[1280:1920, :],
        NT,
        preferred_element_type=F32,
    )
    place(mid_ref, value, 2, 9)
    leave(mid_ref, out_two)
    left = jnp.concatenate(left[:4], axis=0)
    for n in range(5):
        columns = slice(256 * n, 256 * n + 256)
        value = lax.dot_general(left, table_ref[columns, :], NT, preferred_element_type=F32)
        place(big_ref.at[n], value, 4, 19)
        leave(big_ref.at[n], out_one.at[:, :, pl.ds(256 * n, 256)])
    for copy in leaving:
        copy.wait()


def call(kernel, out_shape, limit, **kw):
    return pl.pallas_call(
        kernel,
        out_shape=out_shape,
        compiler_params=pltpu.CompilerParams(vmem_limit_bytes=limit * 1024 * 1024),
        **kw,
    )


def on_device(grid_fields, assign, limits, legendre, synth_one, synth_two, synth_three):
    fields, rows, lon = grid_fields.shape
    lat_at = lax.axis_index("lat")
    fld_at = lax.axis_index("fld")
    vmem = pl.BlockSpec(memory_space=pltpu.VMEM)

    hbm = pl.BlockSpec(memory_space=pltpu.HBM)
    own = jnp.transpose(legendre, (0, 2, 1))
    low, high = call(
        pack_kernel,
        [jax.ShapeDtypeStruct((800, 512), BF16)] * 2,
        60,
        in_specs=[hbm],
        out_specs=[hbm, hbm],
        scratch_shapes=[
            pltpu.VMEM((800, 512), BF16),
            pltpu.VMEM((800, 512), BF16),
            pltpu.SemaphoreType.DMA((10,)),
            pltpu.SemaphoreType.DMA((2,)),
        ],
        name="pack",
    )(own)
    low, high, grid_fields, assign = lax.optimization_barrier((low, high, grid_fields, assign))
    right = [(k, (k + 1) % 4) for k in range(4)]
    left = [(k, (k + 3) % 4) for k in range(4)]
    across = [(k, (k + 2) % 4) for k in range(4)]
    low_left = lax.ppermute(low, "fld", right)
    high_right = lax.ppermute(high, "fld", left)
    low_right = lax.ppermute(low, "fld", left)
    high_left = lax.ppermute(high, "fld", right)
    low_far = lax.ppermute(low_left, "fld", right)
    high_far = lax.ppermute(high_right, "fld", left)

    pairs = assign.reshape(32, 10)
    even = jnp.where(pairs % 2 == 0, pairs, 639 - pairs).astype(F32)
    odd = 639.0 - even
    spare = jnp.zeros((32, 4), F32)
    forward_waves = jnp.stack(
        [
            jnp.concatenate([even, even, spare], axis=1),
            jnp.concatenate([spare, odd, odd], axis=1),
        ]
    ).reshape(2, 768)
    wire = call(
        dft_kernel,
        jax.ShapeDtypeStruct((32, 40, 1024), BF16),
        60,
        in_specs=[pl.BlockSpec(memory_space=pltpu.SMEM), vmem, hbm],
        out_specs=hbm,
        scratch_shapes=[
            pltpu.VMEM((fields * rows, lon), BF16),
            pltpu.VMEM((32, 40, 1024), BF16),
            pltpu.VMEM((lon // 2, 768), BF16),
            pltpu.VMEM((lon // 2, 768), BF16),
            pltpu.VMEM((1024, lon // 2), BF16),
            pltpu.VMEM((1024, lon // 2), BF16),
            pltpu.VMEM((384, lon // 2), BF16),
            pltpu.VMEM((80, 768), F32),
            pltpu.VMEM((80, 768), F32),
            pltpu.SemaphoreType.DMA(()),
            pltpu.SemaphoreType.DMA((2,)),
        ],
        name="dft",
    )((lat_at % 16 * 40).reshape(1), forward_waves, grid_fields.reshape(fields * rows, lon))
    assign_after, synth_one, synth_two, synth_three, own, wire = lax.optimization_barrier(
        (assign, synth_one, synth_two, synth_three, own, wire)
    )
    wire = lax.all_to_all(wire, "lat", split_axis=0, concat_axis=0, tiled=True)

    rest = call(
        pack_rest_kernel,
        jax.ShapeDtypeStruct((1760, 128), BF16),
        60,
        in_specs=[hbm],
        out_specs=hbm,
        scratch_shapes=[
            pltpu.VMEM((1760, 128), BF16),
            pltpu.VMEM((10, 160, 1), BF16),
            pltpu.SemaphoreType.DMA((11,)),
            pltpu.SemaphoreType.DMA(()),
        ],
        name="pack_rest",
    )(own)
    rest_left = lax.ppermute(rest, "fld", right)
    rest_right = lax.ppermute(rest, "fld", left)
    rest_far = lax.ppermute(rest, "fld", across)

    synths = (synth_one, synth_two, synth_three)
    slot_block = [pl.BlockSpec((1,) + t.shape[1:], lambda q: (q, 0, 0)) for t in synths]
    turned = call(
        turn_tables_kernel,
        [jax.ShapeDtypeStruct(t.shape, BF16) for t in synths],
        60,
        grid=(10,),
        in_specs=slot_block,
        out_specs=slot_block,
        scratch_shapes=[pltpu.VMEM(t.shape[1:], BF16) for t in synths],
        name="turn_tables",
    )(*synths)

    info = jnp.concatenate(
        [fld_at.reshape(1), lax.dynamic_slice_in_dim(assign_after, lat_at * 10, 10), limits]
    )
    spectrum, level_wire, waves = call(
        level_kernel,
        [
            jax.ShapeDtypeStruct((10, 2 * fields, 512), BF16),
            jax.ShapeDtypeStruct((32, 144, 128), BF16),
            jax.ShapeDtypeStruct((10, 192, 640), BF16),
        ],
        60,
        in_specs=[pl.BlockSpec(memory_space=pltpu.SMEM)] + [hbm] * 12,
        out_specs=[hbm, hbm, hbm],
        scratch_shapes=[
            pltpu.VMEM((5, fields * rows, 128), F32),
            pltpu.VMEM((5, fields * rows, 128), F32),
            pltpu.VMEM((10, 192, 640), BF16),
            pltpu.VMEM((10, 640, 512), BF16),
        ]
        + [pltpu.VMEM(t.shape, BF16) for t in turned]
        + [
            pltpu.VMEM((10, 2 * fields, 512), BF16),
            pltpu.VMEM((32 * 144, 128), F32),
            pltpu.VMEM((32, 144, 128), BF16),
            pltpu.VMEM((32, 40, 1024), BF16),
            pltpu.SemaphoreType.DMA((2,)),
            pltpu.SemaphoreType.DMA((10, 4)),
            pltpu.SemaphoreType.DMA((3,)),
            pltpu.SemaphoreType.DMA((3,)),
        ],
        name="levels",
    )(
        info,
        wire,
        low,
        low_left,
        low_right,
        low_far,
        high,
        high_left,
        high_right,
        high_far,
        *turned,
    )
    info, waves, level_wire = lax.optimization_barrier((info, waves, level_wire))
    rest_spectrum = call(
        rest_kernel,
        jax.ShapeDtypeStruct((10, 2 * fields, 129), BF16),
        16,
        in_specs=[pl.BlockSpec(memory_space=pltpu.SMEM)] + [vmem] * 5,
        out_specs=vmem,
        scratch_shapes=[pltpu.VMEM((10, 640, 128), BF16), pltpu.VMEM((640, 128), BF16)],
        name="rest",
    )(info, waves, rest, rest_left, rest_right, rest_far)
    level_wire = lax.all_to_all(level_wire, "lat", split_axis=0, concat_axis=0, tiled=True)
    assign_late, rest_spectrum = lax.optimization_barrier((assign, rest_spectrum))
    plain = assign_late.reshape(32, 10).astype(F32)
    spare = jnp.zeros((32, 4), F32)
    inverse_waves = jnp.concatenate([plain, plain, spare], axis=1).reshape(1, 768)
    table = call(
        inverse_table_kernel,
        jax.ShapeDtypeStruct((2240, 768), BF16),
        12,
        in_specs=[vmem],
        out_specs=vmem,
        scratch_shapes=[pltpu.VMEM((80, 768), F32), pltpu.VMEM((80, 768), F32)],
        name="inverse_tables",
    )(inverse_waves)


    late_half = (lat_at >= 16).astype(jnp.int32).reshape(1)
    grids = call(
        inverse_kernel,
        [
            jax.ShapeDtypeStruct((20, fields, 1280), F32),
            jax.ShapeDtypeStruct((10, fields, 640), F32),
            jax.ShapeDtypeStruct((5, fields, 320), F32),
        ],
        24,
        in_specs=[pl.BlockSpec(memory_space=pltpu.SMEM), vmem, vmem],
        out_specs=[hbm] * 3,
        scratch_shapes=[
            pltpu.VMEM((5, 20, fields, 256), F32),
            pltpu.VMEM((10, fields, 640), F32),
            pltpu.VMEM((5, fields, 320), F32),
            pltpu.SemaphoreType.DMA((7,)),
        ],
        name="inverse",
    )(late_half, level_wire, table)
    grids = [jnp.transpose(g, (1, 0, 2)) for g in grids]
    spectrum = jnp.concatenate([spectrum, rest_spectrum], axis=2).reshape(10, 2, fields, 641)
    spectrum = jnp.transpose(spectrum, (2, 1, 0, 3))
    return (spectrum, *grids)


def solution(mesh):
    return jax.shard_map(
        on_device,
        mesh=mesh,
        in_specs=(
            P("fld", "lat", None),
            P(),
            P(),
            P("lat", None, "fld"),
            P("lat", None, None),
            P("lat", None, None),
            P("lat", None, None),
        ),
        out_specs=(
            P("fld", None, "lat", None),
            P("fld", "lat", None),
            P("fld", "lat", None),
            P("fld", "lat", None),
        ),
        check_vma=False,
    )
```

```python
import math

import jax
import jax.numpy as jnp
from jax import lax
from jax.experimental import pallas as pl
from jax.experimental.pallas import tpu as pltpu
from jax.sharding import PartitionSpec as P


F32 = jnp.float32
BF16 = jnp.bfloat16

COS_TERMS = (
    1.0,
    -4.93480110168457,
    4.058694839477539,
    -1.3351584672927856,
    0.23502981662750244,
    -0.025358986109495163,
    0.0015939108561724424,
)
SIN_TERMS = (
    3.141592502593994,
    -5.167698860168457,
    2.5499982833862305,
    -0.5985506176948547,
    0.0807478278875351,
    -0.006089475005865097,
)

NT = (((1,), (1,)), ((), ()))
NN = (((1,), (0,)), ((), ()))


def turn(count, period):
    left = count - period * jnp.floor(count * (1.0 / period) + 0.5)
    place = left * (2.0 / period)
    square = place * place
    cosine = jnp.full_like(square, COS_TERMS[-1])
    for term in COS_TERMS[-2::-1]:
        cosine = cosine * square + term
    sine = jnp.full_like(square, SIN_TERMS[-1])
    for term in SIN_TERMS[-2::-1]:
        sine = sine * square + term
    return cosine, sine * place


def fill_table(wave, shift, scale, high_cos, high_sin, table_ref, period):
    count, width = table_ref.shape
    step = 16
    many = count // step
    low = lax.broadcasted_iota(jnp.int32, (step, width), 0).astype(F32)
    low_cos, low_sin = turn(low * wave, period)
    high = lax.broadcasted_iota(jnp.int32, (many, width), 0).astype(F32)
    first, second = turn(high * (wave * float(step)) + shift, period)
    high_cos[:many, :] = first * scale
    high_sin[:many, :] = second * scale

    def body(k, carry):
        value = high_cos[pl.ds(k, 1), :] * low_cos - high_sin[pl.ds(k, 1), :] * low_sin
        table_ref[pl.ds(pl.multiple_of(k * step, step), step), :] = value.astype(BF16)
        return carry

    lax.fori_loop(0, many, body, 0, unroll=4)


def identity(size):
    across = lax.broadcasted_iota(jnp.int32, (size, size), 0)
    along = lax.broadcasted_iota(jnp.int32, (size, size), 1)
    return jnp.where(across == along, 1.0, 0.0).astype(BF16)


def dft_kernel(
    info_ref,
    waves_ref,
    grid_hbm,
    wire_hbm,
    grid_ref,
    out_ref,
    even_ref,
    odd_ref,
    add_ref,
    sub_ref,
    turned_ref,
    high_cos,
    high_sin,
    in_sem,
    out_sem,
):
    half = grid_hbm.shape[1] // 2
    rows = grid_hbm.shape[0]
    incoming = pltpu.make_async_copy(grid_hbm, grid_ref, in_sem)
    incoming.start()
    lane = lax.broadcasted_iota(jnp.int32, (1, 768), 1).astype(F32)
    lane = lane - 24.0 * jnp.floor((lane + 0.5) * (1.0 / 24.0))
    size = 1.0 / math.sqrt(2 * half)
    for at, table_ref, first in ((0, even_ref, 0.0), (1, odd_ref, 4.0)):
        valid = (lane >= first) & (lane < first + 20.0)
        fill_table(
            waves_ref[at : at + 1, :],
            jnp.where(lane >= first + 10.0, half / 2.0, 0.0),
            jnp.where(valid, size, 0.0),
            high_cos,
            high_sin,
            table_ref,
            2 * half,
        )
    incoming.wait()

    def fold(k, carry):
        part = pl.ds(pl.multiple_of(k * 64, 64), 64)
        first = grid_ref[part, :half].astype(F32)
        second = grid_ref[part, half:].astype(F32)
        add_ref[part, :] = (first + second).astype(BF16)
        sub_ref[part, :] = (first - second).astype(BF16)
        return carry

    lax.fori_loop(0, rows // 64, fold, 0)
    add_ref[rows:, :] = jnp.zeros((1024 - rows, half), BF16)
    sub_ref[rows:, :] = jnp.zeros((1024 - rows, half), BF16)
    same = identity(128)
    turn_by = info_ref[0]
    shift = lax.rem(turn_by, 128)
    tile_shift = lax.div(turn_by, 128)
    lane = lax.broadcasted_iota(jnp.int32, (40, 128), 1)
    for at, table_ref, folded_ref in ((0, even_ref, add_ref), (768, odd_ref, sub_ref)):
        turned_ref[:, at : at + 768] = lax.dot_general(
            folded_ref[...], table_ref[...], NN, preferred_element_type=F32
        ).astype(BF16)
    leaving = []
    for k in range(2):
        even, odd = (
            jnp.concatenate(
                [
                    lax.dot_general(
                        same,
                        turned_ref[:, at + 128 * t : at + 128 * t + 128],
                        NT,
                        preferred_element_type=F32,
                    )
                    for t in range(3)
                ],
                axis=0,
            )
            for at in (384 * k, 768 + 384 * k)
        )
        for d in range(16):
            one = even[24 * d : 24 * d + 24]
            two = odd[24 * d : 24 * d + 24]
            value = jnp.concatenate([one[:16], one[16:] + two[:8], two[8:]], axis=0)
            tiles = [pltpu.roll(value[:, 128 * t : 128 * t + 128], shift, 1) for t in range(8)]
            for t in range(8):
                tile = jnp.where(lane < shift, tiles[t - 1], tiles[t])
                place = pl.multiple_of(lax.rem(tile_shift + t, 8) * 128, 128)
                out_ref[16 * k + d, :, pl.ds(place, 128)] = tile.astype(BF16)
            if d % 8 == 7:
                part = pl.ds(16 * k + d - 7, 8)
                leaving.append(
                    pltpu.make_async_copy(
                        out_ref.at[part], wire_hbm.at[part], out_sem.at[2 * k + d // 8]
                    )
                )
                leaving[-1].start()
    for copy in leaving:
        copy.wait()


def pack_kernel(block_hbm, low_hbm, high_hbm, low_ref, high_ref, in_sem, out_sem):
    incoming = []
    for q in range(10):
        target = low_ref if q < 5 else high_ref
        incoming.append(
            pltpu.make_async_copy(
                block_hbm.at[q, :, pl.ds(0, 512)],
                target.at[pl.ds(q % 5 * 160, 160), :],
                in_sem.at[q],
            )
        )
        incoming[-1].start()
    for copy in incoming[:5]:
        copy.wait()
    low_out = pltpu.make_async_copy(low_ref, low_hbm, out_sem.at[0])
    low_out.start()
    for copy in incoming[5:]:
        copy.wait()
    high_out = pltpu.make_async_copy(high_ref, high_hbm, out_sem.at[1])
    high_out.start()
    low_out.wait()
    high_out.wait()


def pack_rest_kernel(block_hbm, rest_hbm, rest_ref, edge_ref, in_sem, out_sem):
    edge = pltpu.make_async_copy(block_hbm.at[:, :, pl.ds(640, 1)], edge_ref, in_sem.at[10])
    edge.start()
    incoming = []
    for q in range(10):
        incoming.append(
            pltpu.make_async_copy(
                block_hbm.at[q, :, pl.ds(512, 128)],
                rest_ref.at[pl.ds(q * 160, 160), :],
                in_sem.at[q],
            )
        )
        incoming[-1].start()
    edge.wait()
    lane = lax.broadcasted_iota(jnp.int32, (160, 128), 1)
    last = jnp.zeros((160, 128), F32)
    for q in range(10):
        last = jnp.where(lane == q, edge_ref[q].astype(F32), last)
    rest_ref[1600:, :] = last.astype(BF16)
    for copy in incoming:
        copy.wait()
    leaving = pltpu.make_async_copy(rest_ref, rest_hbm, out_sem)
    leaving.start()
    leaving.wait()


def turn_tables_kernel(one_ref, two_ref, three_ref, out_one, out_two, out_three, *picks):
    levels = ((one_ref, out_one, 4), (two_ref, out_two, 2), (three_ref, out_three, 1))

    @pl.when(pl.program_id(0) == 0)
    def _():
        for pick_ref, (source, _, groups) in zip(picks, levels):
            size = source.shape[1]
            row = lax.broadcasted_iota(jnp.int32, (size, size), 0)
            column = lax.broadcasted_iota(jnp.int32, (size, size), 1)
            b = row // (16 * groups)
            a = (row // 16) % groups
            place = (row % 16) * (5 * groups) + 5 * a + b
            pick_ref[...] = jnp.where(place == column, 1.0, 0.0).astype(BF16)

    for pick_ref, (source, target, _) in zip(picks, levels):
        target[0] = lax.dot_general(
            pick_ref[...], source[0], NT, preferred_element_type=F32
        ).astype(BF16)


def row_mask(condition, rows):
    value = jnp.where(condition, 1, 0)
    return jnp.broadcast_to(value, (rows, value.shape[1])) == 1


def level_kernel(
    info_ref,
    arrived_hbm,
    own_low,
    left_low,
    right_low,
    far_low,
    own_high,
    left_high,
    right_high,
    far_high,
    one_hbm,
    two_hbm,
    three_hbm,
    spectrum_hbm,
    wire_hbm,
    waves_hbm,
    north_ref,
    south_ref,
    waves_ref,
    block_ref,
    one_ref,
    two_ref,
    three_ref,
    spectrum_ref,
    pack_ref,
    wire_ref,
    arrived_ref,
    arrived_sem,
    block_sem,
    table_sem,
    spectrum_sem,
    out_sem,
):
    x = info_ref[0]
    arriving = [
        pltpu.make_async_copy(
            arrived_hbm.at[pl.ds(16 * k, 16)], arrived_ref.at[pl.ds(16 * k, 16)], arrived_sem.at[k]
        )
        for k in range(2)
    ]
    for copy in arriving:
        copy.start()
    lows = (own_low, right_low, far_low, left_low)
    highs = (own_high, right_high, far_high, left_high)

    def block_copy(source, q, place, k):
        return pltpu.make_async_copy(
            source.at[pl.ds(q % 5 * 160, 160), :],
            block_ref.at[q, pl.ds(place, 160), :],
            block_sem.at[q, k],
        )

    tables = [
        pltpu.make_async_copy(source, target, table_sem.at[k])
        for k, (source, target) in enumerate(
            ((one_hbm, one_ref), (two_hbm, two_ref), (three_hbm, three_ref))
        )
    ]
    for row in range(140, 144):
        pack_ref[pl.ds(row, 32, stride=144), :] = jnp.zeros((32, 128), F32)

    fields = north_ref.shape[1] // 40
    lane = lax.broadcasted_iota(jnp.int32, (40, 128), 1)
    for half, target in ((0, north_ref), (16, south_ref)):
        arriving[half // 16].wait()
        if half:
            for q in range(10):
                for k, source in enumerate(lows if q < 5 else highs):
                    block_copy(source, q, pl.multiple_of(((x + k) % 4) * 160, 160), k).start()
                if q == 1:
                    for copy in tables:
                        copy.start()
        for f in range(fields):
            offset = 40 * f % 128
            tiles = []
            for o in range(6 if offset else 5):
                at = (40 * f // 128 + o) % 8 * 128
                first = 128 * o - offset
                tile = None
                for k in range(max(first // 40, 0), min((first + 127) // 40, 15) + 1):
                    piece = arrived_ref[half + k, :, at : at + 128]
                    tile = piece if tile is None else jnp.where(lane >= 40 * k - first, piece, tile)
                tiles.append(tile.astype(F32))
            if offset:
                tiles = [pltpu.roll(tile, 128 - offset, 1) for tile in tiles]
                tiles = [
                    jnp.where(lane < 128 - offset, tiles[t], tiles[t + 1]) for t in range(5)
                ]
            for t in range(5):
                target[t, 40 * f : 40 * f + 40, :] = tiles[t]

    across = lax.broadcasted_iota(jnp.int32, (128, 128), 0)
    along = lax.broadcasted_iota(jnp.int32, (128, 128), 1)
    mirror = jnp.where(across + along == 127, 1.0, 0.0).astype(BF16)

    def fold(k, carry):
        rows = pl.ds(pl.multiple_of(k * 96, 96), 96)
        south = [
            lax.dot_general(
                south_ref[4 - t, rows, :].astype(BF16), mirror, NN, preferred_element_type=F32
            )
            for t in range(5)
        ]
        for t in range(5):
            first = north_ref[t, rows, :]
            north_ref[t, rows, :] = first + south[t]
            south_ref[t, rows, :] = first - south[t]
        return carry

    lax.fori_loop(0, north_ref.shape[1] // 96, fold, 0)

    def slot(q, carry):
        for t in range(5):
            parts = [
                source[t, pl.ds(g * 10 + q, fields, stride=40), :]
                for source in (north_ref, south_ref)
                for g in range(4)
            ]
            waves_ref[q, :, 128 * t : 128 * t + 128] = jnp.concatenate(parts, axis=0).astype(BF16)
        return carry

    lax.fori_loop(0, 10, slot, 0)

    waves_out = pltpu.make_async_copy(waves_ref, waves_hbm, out_sem.at[0])
    waves_out.start()
    for copy in tables:
        copy.wait()
    rank = lax.broadcasted_iota(jnp.int32, (1, 512), 1)
    sym = rank < 321
    place = jnp.where(sym, rank, rank - 321)

    def two_slots(step, carry):
        slots = [2 * step, 2 * step + 1]
        orders = [info_ref[1 + q] for q in slots]
        for q in slots:
            for k, source in enumerate(lows):
                pltpu.make_async_copy(
                    source.at[pl.ds(0, 160), :], block_ref.at[q, pl.ds(0, 160), :], block_sem.at[q, k]
                ).wait()
        all_rows = []
        for q, p in zip(slots, orders):
            low = lax.dot_general(
                waves_ref[q, :96, :], block_ref[q, :, :256], NN, preferred_element_type=F32
            )
            high = lax.dot_general(
                waves_ref[q], block_ref[q, :, 256:], NN, preferred_element_type=F32
            )
            bound = jnp.where(sym, (641 - p) // 2, (640 - p) // 2)
            first = row_mask((place < bound) == (p % 2 == 0), 48)
            is_sym = row_mask(sym[:, 256:], 48)
            low = jnp.where(first[:, :256], low[:48], low[48:])
            high = jnp.where(
                is_sym,
                jnp.where(first[:, 256:], high[0:48], high[48:96]),
                jnp.where(first[:, 256:], high[96:144], high[144:192]),
            )
            chosen = jnp.concatenate([low, high], axis=1).astype(BF16)
            spectrum_ref[q] = chosen
            pltpu.make_async_copy(
                spectrum_ref.at[q], spectrum_hbm.at[q], spectrum_sem.at[q]
            ).start()
            all_rows.append(chosen.astype(F32))
        group = 0
        for level, table_ref, count in ((0, one_ref, 4), (1, two_ref, 2), (2, three_ref, 1)):
            size = table_ref.shape[1]
            half = size // 2
            limit = info_ref[11 + level]
            lane = lax.broadcasted_iota(jnp.int32, (1, size), 1)
            is_sym = lane < half
            sym_rows = row_mask(is_sym, 48)
            extra = jnp.where(is_sym, 2 * lane, 2 * (lane - half) + 1)
            many = 16 * count
            wide = lax.broadcasted_iota(jnp.int32, (many, 128), 1)
            for k, (q, p) in enumerate(zip(slots, orders)):
                rows = all_rows[k]
                later = pltpu.roll(rows, 512 - 321 + half, 1)[:, :size]
                keep = row_mask(p + extra <= limit, 48)
                kept = jnp.where(keep, jnp.where(sym_rows, rows[:, :size], later), 0.0)
                both = jnp.concatenate(
                    [kept, jnp.where(sym_rows, kept, -kept), jnp.zeros((32, size), F32)], axis=0
                ).astype(BF16)
                value = lax.dot_general(table_ref[q], both, NT, preferred_element_type=F32)
                for sign in range(2):
                    for c in range(2):
                        packed = None
                        for b in range(5):
                            part = value[many * b : many * b + many]
                            move = 24 * (b - 2 * sign - c) % 128
                            if move:
                                part = pltpu.roll(part, move, 1)
                            packed = part if b == 0 else jnp.where(wide >= 24 * b, part, packed)
                        for a in range(count):
                            start = sign * 16 * 144 + 20 * (group + a) + 10 * c + q
                            pack_ref[pl.ds(start, 16, stride=144), :] = packed[16 * a : 16 * a + 16]
            group += count

        return carry

    lax.fori_loop(0, 5, two_slots, 0)
    for d in range(16):
        wire_ref[d] = pack_ref[144 * d : 144 * d + 144, :].astype(BF16)
        wire_ref[31 - d] = pack_ref[144 * (16 + d) : 144 * (17 + d), :].astype(BF16)
    wire_out = pltpu.make_async_copy(wire_ref, wire_hbm, out_sem.at[1])
    wire_out.start()
    for q in range(10):
        pltpu.make_async_copy(spectrum_ref.at[q], spectrum_hbm.at[q], spectrum_sem.at[q]).wait()
    wire_out.wait()
    waves_out.wait()


def rest_kernel(
    info_ref, waves_ref, own_ref, left_ref, right_ref, far_ref, out_ref, block_ref, edge_ref
):
    x = info_ref[0]
    for k, source in enumerate((own_ref, right_ref, far_ref, left_ref)):
        place = pl.multiple_of(((x + k) % 4) * 160, 160)
        for q in range(10):
            block_ref[q, pl.ds(place, 160), :] = source[160 * q : 160 * q + 160, :]
        edge_ref[pl.ds(place, 160), :] = source[1600:, :]
    rank = lax.broadcasted_iota(jnp.int32, (1, 128), 1) + (512 - 321)
    lane = lax.broadcasted_iota(jnp.int32, (48, 128), 1)

    def slot(q, carry):
        p = info_ref[1 + q]
        left = waves_ref[q, 96:, :]
        even_pair = p % 2 == 0
        bound = (640 - p) // 2
        value = lax.dot_general(left, block_ref[q], NN, preferred_element_type=F32)
        first = row_mask((rank < bound) == even_pair, 48)
        out_ref[q, :, :128] = jnp.where(first, value[:48], value[48:]).astype(BF16)
        value = lax.dot_general(left, edge_ref[...], NN, preferred_element_type=F32)
        value = jnp.where(((319 < bound) == even_pair) & (lane >= 0), value[:48], value[48:])
        out_ref[q, :, 128:] = pltpu.roll(value, lax.rem(128 - q, 128), 1)[:, :1].astype(BF16)
        return carry

    lax.fori_loop(0, 10, slot, 0)


def inverse_table_kernel(waves_ref, table_ref, high_cos, high_sin):
    wave = waves_ref[0:1, :]
    lane = lax.broadcasted_iota(jnp.int32, (1, 768), 1).astype(F32)
    lane = lane - 24.0 * jnp.floor((lane + 0.5) * (1.0 / 24.0))
    weight = jnp.where(lane < 20.0, jnp.where(wave == 0.0, 1.0, 2.0), 0.0)
    first = 0
    for period in (1280, 640, 320):
        shift = jnp.where(lane >= 10.0, period / 4.0, 0.0)
        scale = weight * (1.0 / math.sqrt(period))
        part = table_ref.at[pl.ds(first, period), :]
        fill_table(wave, shift, scale, high_cos, high_sin, part, period)
        first += period


def inverse_kernel(
    info_ref,
    wire_ref,
    table_ref,
    out_one,
    out_two,
    out_three,
    big_ref,
    mid_ref,
    small_ref,
    out_sem,
):
    late_half = info_ref[0]
    same = identity(128)

    def lines(group):
        start = 20 * group // 8 * 8
        part = wire_ref[:, start : start + 24, :].astype(F32)
        if 20 * group > start:
            part = pltpu.roll(part, 24 - (20 * group - start), 1)
        part = part.reshape(part.shape[0] * 24, 128).astype(BF16)
        return lax.dot_general(same, part, NT, preferred_element_type=F32).astype(BF16)

    def place(target, value, count, last):
        for a in range(count):
            for b in range(5):
                row = 5 * a + b
                row = jnp.where(late_half == 1, last - row, row)
                target[row] = value[128 * a + 24 * b : 128 * a + 24 * b + 24]

    leaving = []

    def leave(source, target):
        copy = pltpu.make_async_copy(source, target, out_sem.at[len(leaving)])
        copy.start()
        leaving.append(copy)

    left = [lines(group) for group in range(7)]
    value = lax.dot_general(left[6], table_ref[1920:, :], NT, preferred_element_type=F32)
    place(small_ref, value, 1, 4)
    leave(small_ref, out_three)
    value = lax.dot_general(
        jnp.concatenate(left[4:6], axis=0),
        table_ref[1280:1920, :],
        NT,
        preferred_element_type=F32,
    )
    place(mid_ref, value, 2, 9)
    leave(mid_ref, out_two)
    left = jnp.concatenate(left[:4], axis=0)
    for n in range(5):
        columns = slice(256 * n, 256 * n + 256)
        value = lax.dot_general(left, table_ref[columns, :], NT, preferred_element_type=F32)
        place(big_ref.at[n], value, 4, 19)
        leave(big_ref.at[n], out_one.at[:, :, pl.ds(256 * n, 256)])
    for copy in leaving:
        copy.wait()


def call(kernel, out_shape, limit, **kw):
    return pl.pallas_call(
        kernel,
        out_shape=out_shape,
        compiler_params=pltpu.CompilerParams(vmem_limit_bytes=limit * 1024 * 1024),
        **kw,
    )


def on_device(grid_fields, assign, limits, legendre, synth_one, synth_two, synth_three):
    fields, rows, lon = grid_fields.shape
    lat_at = lax.axis_index("lat")
    fld_at = lax.axis_index("fld")
    vmem = pl.BlockSpec(memory_space=pltpu.VMEM)

    hbm = pl.BlockSpec(memory_space=pltpu.HBM)
    own = jnp.transpose(legendre, (0, 2, 1))
    low, high = call(
        pack_kernel,
        [jax.ShapeDtypeStruct((800, 512), BF16)] * 2,
        60,
        in_specs=[hbm],
        out_specs=[hbm, hbm],
        scratch_shapes=[
            pltpu.VMEM((800, 512), BF16),
            pltpu.VMEM((800, 512), BF16),
            pltpu.SemaphoreType.DMA((10,)),
            pltpu.SemaphoreType.DMA((2,)),
        ],
        name="pack",
    )(own)
    low, high, grid_fields, assign = lax.optimization_barrier((low, high, grid_fields, assign))
    right = [(k, (k + 1) % 4) for k in range(4)]
    left = [(k, (k + 3) % 4) for k in range(4)]
    across = [(k, (k + 2) % 4) for k in range(4)]
    low_left = lax.ppermute(low, "fld", right)
    high_right = lax.ppermute(high, "fld", left)
    low_right = lax.ppermute(low, "fld", left)
    high_left = lax.ppermute(high, "fld", right)
    low_far = lax.ppermute(low_left, "fld", right)
    high_far = lax.ppermute(high_right, "fld", left)

    pairs = assign.reshape(32, 10)
    even = jnp.where(pairs % 2 == 0, pairs, 639 - pairs).astype(F32)
    odd = 639.0 - even
    spare = jnp.zeros((32, 4), F32)
    forward_waves = jnp.stack(
        [
            jnp.concatenate([even, even, spare], axis=1),
            jnp.concatenate([spare, odd, odd], axis=1),
        ]
    ).reshape(2, 768)
    wire = call(
        dft_kernel,
        jax.ShapeDtypeStruct((32, 40, 1024), BF16),
        60,
        in_specs=[pl.BlockSpec(memory_space=pltpu.SMEM), vmem, hbm],
        out_specs=hbm,
        scratch_shapes=[
            pltpu.VMEM((fields * rows, lon), BF16),
            pltpu.VMEM((32, 40, 1024), BF16),
            pltpu.VMEM((lon // 2, 768), BF16),
            pltpu.VMEM((lon // 2, 768), BF16),
            pltpu.VMEM((1024, lon // 2), BF16),
            pltpu.VMEM((1024, lon // 2), BF16),
            pltpu.VMEM((1024, 1536), BF16),
            pltpu.VMEM((80, 768), F32),
            pltpu.VMEM((80, 768), F32),
            pltpu.SemaphoreType.DMA(()),
            pltpu.SemaphoreType.DMA((4,)),
        ],
        name="dft",
    )((lat_at % 16 * 40).reshape(1), forward_waves, grid_fields.reshape(fields * rows, lon))
    assign_after, synth_one, synth_two, synth_three, own, wire = lax.optimization_barrier(
        (assign, synth_one, synth_two, synth_three, own, wire)
    )
    wire = lax.all_to_all(wire, "lat", split_axis=0, concat_axis=0, tiled=True)

    rest = call(
        pack_rest_kernel,
        jax.ShapeDtypeStruct((1760, 128), BF16),
        60,
        in_specs=[hbm],
        out_specs=hbm,
        scratch_shapes=[
            pltpu.VMEM((1760, 128), BF16),
            pltpu.VMEM((10, 160, 1), BF16),
            pltpu.SemaphoreType.DMA((11,)),
            pltpu.SemaphoreType.DMA(()),
        ],
        name="pack_rest",
    )(own)
    rest_left = lax.ppermute(rest, "fld", right)
    rest_right = lax.ppermute(rest, "fld", left)
    rest_far = lax.ppermute(rest, "fld", across)

    synths = (synth_one, synth_two, synth_three)
    slot_block = [pl.BlockSpec((1,) + t.shape[1:], lambda q: (q, 0, 0)) for t in synths]
    turned = call(
        turn_tables_kernel,
        [jax.ShapeDtypeStruct(t.shape, BF16) for t in synths],
        60,
        grid=(10,),
        in_specs=slot_block,
        out_specs=slot_block,
        scratch_shapes=[pltpu.VMEM(t.shape[1:], BF16) for t in synths],
        name="turn_tables",
    )(*synths)

    info = jnp.concatenate(
        [fld_at.reshape(1), lax.dynamic_slice_in_dim(assign_after, lat_at * 10, 10), limits]
    )
    spectrum, level_wire, waves = call(
        level_kernel,
        [
            jax.ShapeDtypeStruct((10, 2 * fields, 512), BF16),
            jax.ShapeDtypeStruct((32, 144, 128), BF16),
            jax.ShapeDtypeStruct((10, 192, 640), BF16),
        ],
        60,
        in_specs=[pl.BlockSpec(memory_space=pltpu.SMEM)] + [hbm] * 12,
        out_specs=[hbm, hbm, hbm],
        scratch_shapes=[
            pltpu.VMEM((5, fields * rows, 128), F32),
            pltpu.VMEM((5, fields * rows, 128), F32),
            pltpu.VMEM((10, 192, 640), BF16),
            pltpu.VMEM((10, 640, 512), BF16),
        ]
        + [pltpu.VMEM(t.shape, BF16) for t in turned]
        + [
            pltpu.VMEM((10, 2 * fields, 512), BF16),
            pltpu.VMEM((32 * 144, 128), F32),
            pltpu.VMEM((32, 144, 128), BF16),
            pltpu.VMEM((32, 40, 1024), BF16),
            pltpu.SemaphoreType.DMA((2,)),
            pltpu.SemaphoreType.DMA((10, 4)),
            pltpu.SemaphoreType.DMA((3,)),
            pltpu.SemaphoreType.DMA((10,)),
            pltpu.SemaphoreType.DMA((2,)),
        ],
        name="levels",
    )(
        info,
        wire,
        low,
        low_left,
        low_right,
        low_far,
        high,
        high_left,
        high_right,
        high_far,
        *turned,
    )
    info, waves, level_wire = lax.optimization_barrier((info, waves, level_wire))
    rest_spectrum = call(
        rest_kernel,
        jax.ShapeDtypeStruct((10, 2 * fields, 129), BF16),
        16,
        in_specs=[pl.BlockSpec(memory_space=pltpu.SMEM)] + [vmem] * 5,
        out_specs=vmem,
        scratch_shapes=[pltpu.VMEM((10, 640, 128), BF16), pltpu.VMEM((640, 128), BF16)],
        name="rest",
    )(info, waves, rest, rest_left, rest_right, rest_far)
    level_wire = lax.all_to_all(level_wire, "lat", split_axis=0, concat_axis=0, tiled=True)
    assign_late, rest_spectrum = lax.optimization_barrier((assign, rest_spectrum))
    plain = assign_late.reshape(32, 10).astype(F32)
    spare = jnp.zeros((32, 4), F32)
    inverse_waves = jnp.concatenate([plain, plain, spare], axis=1).reshape(1, 768)
    table = call(
        inverse_table_kernel,
        jax.ShapeDtypeStruct((2240, 768), BF16),
        12,
        in_specs=[vmem],
        out_specs=vmem,
        scratch_shapes=[pltpu.VMEM((80, 768), F32), pltpu.VMEM((80, 768), F32)],
        name="inverse_tables",
    )(inverse_waves)


    late_half = (lat_at >= 16).astype(jnp.int32).reshape(1)
    grids = call(
        inverse_kernel,
        [
            jax.ShapeDtypeStruct((20, fields, 1280), F32),
            jax.ShapeDtypeStruct((10, fields, 640), F32),
            jax.ShapeDtypeStruct((5, fields, 320), F32),
        ],
        24,
        in_specs=[pl.BlockSpec(memory_space=pltpu.SMEM), vmem, vmem],
        out_specs=[hbm] * 3,
        scratch_shapes=[
            pltpu.VMEM((5, 20, fields, 256), F32),
            pltpu.VMEM((10, fields, 640), F32),
            pltpu.VMEM((5, fields, 320), F32),
            pltpu.SemaphoreType.DMA((7,)),
        ],
        name="inverse",
    )(late_half, level_wire, table)
    grids = [jnp.transpose(g, (1, 0, 2)) for g in grids]
    spectrum = jnp.concatenate([spectrum, rest_spectrum], axis=2).reshape(10, 2, fields, 641)
    spectrum = jnp.transpose(spectrum, (2, 1, 0, 3))
    return (spectrum, *grids)


def solution(mesh):
    return jax.shard_map(
        on_device,
        mesh=mesh,
        in_specs=(
            P("fld", "lat", None),
            P(),
            P(),
            P("lat", None, "fld"),
            P("lat", None, None),
            P("lat", None, None),
            P("lat", None, None),
        ),
        out_specs=(
            P("fld", None, "lat", None),
            P("fld", "lat", None),
            P("fld", "lat", None),
            P("fld", "lat", None),
        ),
        check_vma=False,
    )
```
